16 devices in a mesh: rep: 1, dp: 16 (over x, y, z, core).
Axes of the slice: x: 2, y: 2, z: 2, core: 2. Of those that a mesh axis runs over, the one named last changes fastest.
Arguments:
- g_w_gate: bfloat16 [16, 2, 1024, 4096], P(('rep', 'dp'))
- g_w_up: bfloat16 [16, 2, 1024, 4096], P(('rep', 'dp'))
- g_w_down: bfloat16 [16, 2, 4096, 1024], P(('rep', 'dp'))
- w_gate: bfloat16 [2, 1024, 4096], replicated
- w_up: bfloat16 [2, 1024, 4096], replicated
- w_down: bfloat16 [2, 4096, 1024], replicated
- m_w_gate: float32 [2, 1024, 4096], P(None, 'dp')
- m_w_up: float32 [2, 1024, 4096], P(None, 'dp')
- m_w_down: float32 [2, 4096, 1024], P(None, 'dp')
- v_w_gate: float32 [2, 1024, 4096], P(None, 'dp')
- v_w_up: float32 [2, 1024, 4096], P(None, 'dp')
- v_w_down: float32 [2, 4096, 1024], P(None, 'dp')
Outputs:
- output 1: bfloat16 [2, 1024, 4096], P('rep')
- output 2: bfloat16 [2, 1024, 4096], P('rep')
- output 3: bfloat16 [2, 4096, 1024], P('rep')
- output 4: float32 [2, 1024, 4096], P('rep', 'dp')
- output 5: float32 [2, 1024, 4096], P('rep', 'dp')
- output 6: float32 [2, 4096, 1024], P('rep', 'dp')
- output 7: float32 [2, 1024, 4096], P('rep', 'dp')
- output 8: float32 [2, 1024, 4096], P('rep', 'dp')
- output 9: float32 [2, 4096, 1024], P('rep', 'dp')
All inputs are finite; a program needn't handle non-finite values.
Results may differ from the reference program's by a relative error of at most 0.022.
Values are sent between devices in bfloat16 or wider.
A program may use at most 2 GiB of HBM per device.

```python
import jax
import jax.numpy as jnp
from jax import lax

DEVICES = 16
D = 1024
FF = 4096
LAYERS = 2
NAMES = ("w_gate", "w_up", "w_down")
SHAPES = {"w_gate": (LAYERS, D, FF), "w_up": (LAYERS, D, FF), "w_down": (LAYERS, FF, D)}


def setup_inputs(seed: int = 0, part: int = 0) -> dict:
    kz, *keys = jax.random.split(jax.random.key(seed), 1 + 5 * len(NAMES))
    loud = 2.0 ** jax.random.uniform(kz, (), jnp.float32, -1.0, 1.0)
    drawn = {}
    for name, key, both in zip(NAMES, keys[:3], keys[3:6], strict=True):
        own = jax.random.normal(jax.random.fold_in(key, part), (DEVICES, *SHAPES[name]), jnp.float32)
        shared = jax.random.normal(jax.random.fold_in(both, part), SHAPES[name], jnp.float32)
        drawn["g_" + name] = (loud * (0.7 * shared / DEVICES + 0.7 * own * DEVICES**-0.5)).astype(jnp.bfloat16)
    for name, key in zip(NAMES, keys[6:9], strict=True):
        drawn[name] = (jax.random.normal(key, SHAPES[name], jnp.float32) * SHAPES[name][1] ** -0.5).astype(jnp.bfloat16)
    for name, key in zip(NAMES, keys[9:12], strict=True):
        drawn["m_" + name] = loud * 0.5 * jax.random.normal(key, SHAPES[name], jnp.float32)
    for name, key in zip(NAMES, keys[12:15], strict=True):
        drawn["v_" + name] = loud * loud * jax.random.uniform(key, SHAPES[name], jnp.float32, 0.5, 1.5)
    return drawn


def adamw(w, m, v, g):
    m = 0.9 * m + 0.1 * g
    v = 0.95 * v + 0.05 * g * g
    step = m * lax.rsqrt(v + 1e-8) + 0.1 * w
    return (w - 0.02 * step).astype(jnp.bfloat16), m, v


def clipped(gradients, sum_of_squares, count):
    factor = jnp.minimum(1.0, 0.5 * lax.rsqrt(sum_of_squares / count + 1e-30))
    return [g * factor for g in gradients]


def reference(g_w_gate, g_w_up, g_w_down, w_gate, w_up, w_down, m_w_gate, m_w_up, m_w_down, v_w_gate, v_w_up, v_w_down):
    def total(terms):
        return lax.scan(lambda so_far, term: (so_far + term.astype(jnp.float32), None), jnp.zeros(terms.shape[1:], jnp.float32), terms)[0]

    gradients = [total(terms).astype(jnp.bfloat16).astype(jnp.float32) for terms in (g_w_gate, g_w_up, g_w_down)]
    gradients = clipped(gradients, sum(jnp.sum(g * g) for g in gradients), sum(g.size for g in gradients))
    new = [
        adamw(w.astype(jnp.float32), m, v, g)
        for w, m, v, g in zip((w_gate, w_up, w_down), (m_w_gate, m_w_up, m_w_down), (v_w_gate, v_w_up, v_w_down), gradients, strict=True)
    ]
    return tuple(one[which] for which in range(3) for one in new)
```

```python
import functools

import jax
import jax.numpy as jnp
from jax import lax
from jax.experimental import pallas as pl
from jax.experimental.pallas import tpu as pltpu
from jax.sharding import PartitionSpec as P

MESH = pl.DeviceIdType.MESH
BF16, F32 = jnp.bfloat16, jnp.float32
DEVICES = 16
LAYERS = 2
CHUNKS = 4
JOBS = LAYERS * CHUNKS
ORDERS = ("xyz", "yzx", "zxy")
STEP = {"x": 8, "y": 4, "z": 2, "c": 1}


def adamw(w, m, v, g):
    m = 0.9 * m + 0.1 * g
    v = 0.95 * v + 0.05 * g * g
    step = m * lax.rsqrt(v + 1e-8) + 0.1 * w
    return (w - 0.02 * step).astype(jnp.bfloat16), m, v


def place(me):
    bit = {a: (me // s) % 2 for a, s in STEP.items()}
    peer = {a: me + s - 2 * s * bit[a] for a, s in STEP.items()}
    return bit, peer


def greet(me):
    barrier = pltpu.get_barrier_semaphore()
    for i in range(1, DEVICES):
        pl.semaphore_signal(barrier, inc=1, device_id={"dp": (me + i) % DEVICES}, device_id_type=MESH)
    pl.semaphore_wait(barrier, DEVICES - 1)


def send(src, dst, sems, to):
    return pltpu.make_async_remote_copy(src, dst, sems[0], sems[1], device_id={"dp": to}, device_id_type=MESH)


def at_axis(ref, lead, axes, axis, bit):
    where = tuple(bit if a == axis else slice(None) for a in axes)
    return ref.at[(*lead, *where)]


def scatter_kernel(*refs):
    g, refs = refs[:3], refs[3:]
    out, total, refs = refs[:3], refs[3], refs[4:]
    own, s0, r1, r2, r3, gb, acc = (refs[3 * i : 3 * i + 3] for i in range(7))
    mine, all_sq, own_sem, out_sem, tx, rx, sq_tx, sq_rx = refs[21:]
    me = lax.axis_index("dp")
    bit, peer = place(me)
    shapes = [r.shape[-2:] for r in r3]

    def rows(k, j):
        h = shapes[k][0]
        return j // CHUNKS, pl.ds((j % CHUNKS) * h, h)

    def own_copy(k, j):
        layer, part = rows(k, j)
        return pltpu.make_async_copy(g[k].at[layer, :, :, :, bit["c"], part], own[k].at[j % 3], own_sem.at[k, j])

    def hop(k, stage, j):
        sems = (tx.at[stage, k, j], rx.at[stage, k, j])
        a1, a2, a3 = ORDERS[k]
        if stage == 0:
            layer, part = rows(k, j)
            return send(g[k].at[layer, :, :, :, 1 - bit["c"], part], s0[k].at[j], sems, peer["c"])
        if stage == 1:
            return send(at_axis(s0[k], (j,), "xyz", a1, 1 - bit[a1]), r1[k].at[j], sems, peer[a1])
        if stage == 2:
            rest = [a for a in "xyz" if a != a1]
            return send(at_axis(r1[k], (j,), rest, a2, 1 - bit[a2]), r2[k].at[j], sems, peer[a2])
        return send(r2[k].at[j, 1 - bit[a3]], r3[k].at[j], sems, peer[a3])

    def plus(a, b):
        return (a.astype(F32) + b.astype(F32)).astype(BF16)

    def out_copy(k, j):
        layer, part = rows(k, j)
        return pltpu.make_async_copy(gb[k].at[layer, part], out[k].at[layer, part], out_sem.at[k, j])

    greet(me)
    for k in range(3):
        acc[k][...] = jnp.zeros_like(acc[k])
        for j in range(2):
            own_copy(k, j).start()
            hop(k, 0, j).start()

    def turn(s, _):
        @pl.when(s < JOBS - 2)
        def _():
            for k in range(3):
                own_copy(k, s + 2).start()
                hop(k, 0, s + 2).start()

        @pl.when(s < JOBS)
        def _():
            for k in range(3):
                own_copy(k, s).wait()
                hop(k, 0, s).wait_recv()

                @pl.loop(0, 8)
                def _(b):
                    i = (b // 4, (b // 2) % 2, b % 2)
                    s0[k][(s, *i)] = plus(own[k][(s % 3, *i)], s0[k][(s, *i)])

                hop(k, 1, s).start()

        @pl.when((s >= 1) & (s < JOBS + 1))
        def _():
            j = s - 1
            for k in range(3):
                a1 = ORDERS[k][0]
                hop(k, 1, j).wait_recv()

                @pl.loop(0, 4)
                def _(b):
                    i = [b // 2, b % 2]
                    full = list(i)
                    full.insert("xyz".index(a1), bit[a1])
                    r1[k][(j, *i)] = plus(s0[k][(j, *full)], r1[k][(j, *i)])

                hop(k, 2, j).start()

        @pl.when((s >= 2) & (s < JOBS + 2))
        def _():
            j = s - 2
            for k in range(3):
                a1, a2, _a3 = ORDERS[k]
                rest = [a for a in "xyz" if a != a1]
                hop(k, 2, j).wait_recv()

                @pl.loop(0, 2)
                def _(b):
                    full = [b]
                    full.insert(rest.index(a2), bit[a2])
                    r2[k][j, b] = plus(r1[k][(j, *full)], r2[k][j, b])

                hop(k, 3, j).start()

        @pl.when(s >= 3)
        def _():
            j = s - 3
            for k in range(3):
                a3 = ORDERS[k][2]
                hop(k, 3, j).wait_recv()
                done = plus(r2[k][j, bit[a3]], r3[k][j])
                layer, part = rows(k, j)
                gb[k][layer, part] = done
                wide = done.astype(F32)
                squares = wide * wide
                acc[k][...] += sum(squares[8 * i : 8 * i + 8] for i in range(shapes[k][0] // 8))
                out_copy(k, j).start()

        return 0

    lax.fori_loop(0, JOBS + 3, turn, 0)

    part = jnp.zeros((8, 128), F32)
    for k in range(3):
        a = acc[k][...]
        part += sum(a[:, 128 * i : 128 * i + 128] for i in range(a.shape[1] // 128))
    mine[...] = part
    all_sq[me] = part
    sends = [send(mine, all_sq.at[me], (sq_tx.at[i], sq_rx.at[i]), (me + i) % DEVICES) for i in range(1, DEVICES)]
    for one in sends:
        one.start()
    for one in sends:
        one.wait()
    total[...] = jnp.full((8, 128), jnp.sum(sum(all_sq[i] for i in range(DEVICES))), F32)

    def drain(j, _):
        for k in range(3):
            for stage in range(4):
                hop(k, stage, j).wait_send()
            out_copy(k, j).wait()
        return 0

    lax.fori_loop(0, JOBS, drain, 0)


def scatter(terms):
    blocks = [(t.shape[1] // DEVICES, t.shape[2]) for t in terms]
    split = [t.reshape(LAYERS, 2, 2, 2, 2, *b) for t, b in zip(terms, blocks, strict=True)]
    piece = [(r // CHUNKS, c) for r, c in blocks]
    sem = pltpu.SemaphoreType.DMA
    anywhere = pl.BlockSpec(memory_space=pl.ANY)
    scratch = [pltpu.VMEM((n, *lead, *p), BF16) for n, lead in ((3, (2, 2, 2)), (JOBS, (2, 2, 2)), (JOBS, (2, 2)), (JOBS, (2,)), (JOBS, ())) for p in piece]
    scratch += [pltpu.VMEM((LAYERS, *b), BF16) for b in blocks]
    scratch += [pltpu.VMEM((8, c), F32) for _, c in blocks]
    scratch += [pltpu.VMEM((8, 128), F32), pltpu.VMEM((DEVICES, 8, 128), F32)]
    scratch += [sem((3, JOBS)), sem((3, JOBS)), sem((4, 3, JOBS)), sem((4, 3, JOBS)), sem((DEVICES,)), sem((DEVICES,))]
    *sums, total = pl.pallas_call(
        scatter_kernel,
        out_shape=[jax.ShapeDtypeStruct((LAYERS, *b), BF16) for b in blocks] + [jax.ShapeDtypeStruct((8, 128), F32)],
        in_specs=[anywhere] * 3,
        out_specs=[anywhere] * 3 + [pl.BlockSpec(memory_space=pltpu.VMEM)],
        scratch_shapes=scratch,
        compiler_params=pltpu.CompilerParams(collective_id=0, has_side_effects=True, vmem_limit_bytes=62 * 2**20),
        name="scatter",
    )(*split)
    return sums, total[0, 0]


def solution(mesh):
    def step(*arrays):
        terms, weights, m, v = (arrays[i : i + 3] for i in (0, 3, 6, 9))
        sums, squares = scatter([t[0] for t in terms])
        count = DEVICES * sum(g.size for g in sums)
        factor = jnp.minimum(1.0, 0.5 * lax.rsqrt(squares / count + 1e-30))
        gradients = [g.astype(F32) * factor for g in sums]
        me = lax.axis_index("dp")
        own = [lax.dynamic_slice_in_dim(w, me * one.shape[1], one.shape[1], 1).astype(jnp.float32) for w, one in zip(weights, m, strict=True)]
        new = [adamw(w, m, v, g) for w, m, v, g in zip(own, m, v, gradients, strict=True)]
        whole = [lax.all_gather(one[0], "dp", axis=1, tiled=True) for one in new]
        return (*whole, *(one[1] for one in new), *(one[2] for one in new))

    all_of, cut = P(None, None, None), P(None, "dp", None)
    return jax.shard_map(
        step,
        mesh=mesh,
        in_specs=(P(("rep", "dp"), None, None, None),) * 3 + (all_of,) * 3 + (cut,) * 6,
        out_specs=(P("rep", None, None),) * 3 + (P("rep", "dp", None),) * 6,
        check_vma=False,
    )
```

```python
import functools

import jax
import jax.numpy as jnp
from jax import lax
from jax.experimental import pallas as pl
from jax.experimental.pallas import tpu as pltpu
from jax.sharding import PartitionSpec as P

MESH = pl.DeviceIdType.MESH
BF16, F32 = jnp.bfloat16, jnp.float32
DEVICES = 16
LAYERS = 2
CHUNKS = 4
JOBS = LAYERS * CHUNKS
ORDERS = ("xyz", "yzx", "zxy")
SPACES = (pltpu.VMEM, pltpu.VMEM, pltpu.HBM)
STEP = {"x": 8, "y": 4, "z": 2, "c": 1}


def adamw(w, m, v, g):
    m = 0.9 * m + 0.1 * g
    v = 0.95 * v + 0.05 * g * g
    step = m * lax.rsqrt(v + 1e-8) + 0.1 * w
    return (w - 0.02 * step).astype(jnp.bfloat16), m, v


def place(me):
    bit = {a: (me // s) % 2 for a, s in STEP.items()}
    peer = {a: me + s - 2 * s * bit[a] for a, s in STEP.items()}
    return bit, peer


def greet(me):
    barrier = pltpu.get_barrier_semaphore()
    for i in range(1, DEVICES):
        pl.semaphore_signal(barrier, inc=1, device_id={"dp": (me + i) % DEVICES}, device_id_type=MESH)
    pl.semaphore_wait(barrier, DEVICES - 1)


def send(src, dst, sems, to):
    return pltpu.make_async_remote_copy(src, dst, sems[0], sems[1], device_id={"dp": to}, device_id_type=MESH)


def at_axis(ref, lead, axes, axis, bit):
    where = tuple(bit if a == axis else slice(None) for a in axes)
    return ref.at[(*lead, *where)]


def scatter_kernel(*refs):
    g, refs = refs[:3], refs[3:]
    out, total, refs = refs[:3], refs[3], refs[4:]
    own, s0, r1, r2, r3, gb, acc = (refs[3 * i : 3 * i + 3] for i in range(7))
    mine, all_sq, own_sem, out_sem, tx, rx, sq_tx, sq_rx = refs[21:]
    me = lax.axis_index("dp")
    bit, peer = place(me)
    shapes = [r.shape[-2:] for r in r3]

    def rows(k, j):
        h = shapes[k][0]
        return j // CHUNKS, pl.ds((j % CHUNKS) * h, h)

    def own_copy(k, j):
        layer, part = rows(k, j)
        return pltpu.make_async_copy(g[k].at[layer, :, :, :, bit["c"], part], own[k].at[j % 3], own_sem.at[k, j])

    def hop(k, stage, j):
        sems = (tx.at[stage, k, j], rx.at[stage, k, j])
        a1, a2, a3 = ORDERS[k]
        if stage == 0:
            layer, part = rows(k, j)
            return send(g[k].at[layer, :, :, :, 1 - bit["c"], part], s0[k].at[j], sems, peer["c"])
        if stage == 1:
            return send(at_axis(s0[k], (j,), "xyz", a1, 1 - bit[a1]), r1[k].at[j], sems, peer[a1])
        if stage == 2:
            rest = [a for a in "xyz" if a != a1]
            return send(at_axis(r1[k], (j,), rest, a2, 1 - bit[a2]), r2[k].at[j], sems, peer[a2])
        return send(r2[k].at[j, 1 - bit[a3]], r3[k].at[j], sems, peer[a3])

    def plus(a, b):
        return (a.astype(F32) + b.astype(F32)).astype(BF16)

    def out_copy(k, j):
        layer, part = rows(k, j)
        return pltpu.make_async_copy(gb[k].at[layer, part], out[k].at[layer, part], out_sem.at[k, j])

    greet(me)
    for k in range(3):
        acc[k][...] = jnp.zeros_like(acc[k])
        for j in range(2):
            own_copy(k, j).start()
            hop(k, 0, j).start()

    def turn(s, _):
        @pl.when(s < JOBS - 2)
        def _():
            for k in range(3):
                own_copy(k, s + 2).start()
                hop(k, 0, s + 2).start()

        @pl.when(s < JOBS)
        def _():
            for k in range(3):
                own_copy(k, s).wait()
                hop(k, 0, s).wait_recv()

                @pl.loop(0, 8)
                def _(b):
                    i = (b // 4, (b // 2) % 2, b % 2)
                    s0[k][(s, *i)] = plus(own[k][(s % 3, *i)], s0[k][(s, *i)])

                hop(k, 1, s).start()

        @pl.when((s >= 1) & (s < JOBS + 1))
        def _():
            j = s - 1
            for k in range(3):
                a1 = ORDERS[k][0]
                hop(k, 1, j).wait_recv()

                @pl.loop(0, 4)
                def _(b):
                    i = [b // 2, b % 2]
                    full = list(i)
                    full.insert("xyz".index(a1), bit[a1])
                    r1[k][(j, *i)] = plus(s0[k][(j, *full)], r1[k][(j, *i)])

                hop(k, 2, j).start()

        @pl.when((s >= 2) & (s < JOBS + 2))
        def _():
            j = s - 2
            for k in range(3):
                a1, a2, _a3 = ORDERS[k]
                rest = [a for a in "xyz" if a != a1]
                hop(k, 2, j).wait_recv()

                @pl.loop(0, 2)
                def _(b):
                    full = [b]
                    full.insert(rest.index(a2), bit[a2])
                    r2[k][j, b] = plus(r1[k][(j, *full)], r2[k][j, b])

                hop(k, 3, j).start()

        @pl.when(s >= 3)
        def _():
            j = s - 3
            for k in range(3):
                a3 = ORDERS[k][2]
                hop(k, 3, j).wait_recv()
                done = plus(r2[k][j, bit[a3]], r3[k][j])
                layer, part = rows(k, j)
                gb[k][layer, part] = done
                wide = done.astype(F32)
                squares = wide * wide
                acc[k][...] += sum(squares[8 * i : 8 * i + 8] for i in range(shapes[k][0] // 8))
                out_copy(k, j).start()

        return 0

    lax.fori_loop(0, JOBS + 3, turn, 0)

    part = jnp.zeros((8, 128), F32)
    for k in range(3):
        a = acc[k][...]
        part += sum(a[:, 128 * i : 128 * i + 128] for i in range(a.shape[1] // 128))
    mine[...] = part
    all_sq[me] = part
    sends = [send(mine, all_sq.at[me], (sq_tx.at[i], sq_rx.at[i]), (me + i) % DEVICES) for i in range(1, DEVICES)]
    for one in sends:
        one.start()
    for one in sends:
        one.wait()
    total[...] = jnp.full((8, 128), jnp.sum(sum(all_sq[i] for i in range(DEVICES))), F32)

    def drain(j, _):
        for k in range(3):
            for stage in range(4):
                hop(k, stage, j).wait_send()
            out_copy(k, j).wait()
        return 0

    lax.fori_loop(0, JOBS, drain, 0)


def scatter(terms):
    blocks = [(t.shape[1] // DEVICES, t.shape[2]) for t in terms]
    split = [t.reshape(LAYERS, 2, 2, 2, 2, *b) for t, b in zip(terms, blocks, strict=True)]
    piece = [(r // CHUNKS, c) for r, c in blocks]
    sem = pltpu.SemaphoreType.DMA
    anywhere = pl.BlockSpec(memory_space=pl.ANY)
    scratch = [pltpu.VMEM((n, *lead, *p), BF16) for n, lead in ((3, (2, 2, 2)), (JOBS, (2, 2, 2)), (JOBS, (2, 2)), (JOBS, (2,)), (JOBS, ())) for p in piece]
    scratch += [pltpu.VMEM((LAYERS, *b), BF16) for b in blocks]
    scratch += [pltpu.VMEM((8, c), F32) for _, c in blocks]
    scratch += [pltpu.VMEM((8, 128), F32), pltpu.VMEM((DEVICES, 8, 128), F32)]
    scratch += [sem((3, JOBS)), sem((3, JOBS)), sem((4, 3, JOBS)), sem((4, 3, JOBS)), sem((DEVICES,)), sem((DEVICES,))]
    *sums, total = pl.pallas_call(
        scatter_kernel,
        out_shape=[jax.ShapeDtypeStruct((LAYERS, *b), BF16) for b in blocks] + [jax.ShapeDtypeStruct((8, 128), F32)],
        in_specs=[anywhere] * 3,
        out_specs=[anywhere] * 3 + [pl.BlockSpec(memory_space=pltpu.VMEM)],
        scratch_shapes=scratch,
        compiler_params=pltpu.CompilerParams(collective_id=0, has_side_effects=True, vmem_limit_bytes=62 * 2**20),
        name="scatter",
    )(*split)
    return sums, total[0, 0]


def gather_kernel(*refs):
    w, refs = refs[:3], refs[3:]
    whole, (own_sem, own_tx, own_rx, tx, rx, ftx, frx) = refs[:3], refs[3:]
    me = lax.axis_index("dp")
    bit, peer = place(me)
    heights = [r.shape[-2] // CHUNKS for r in whole]

    def own_copy(k):
        return pltpu.make_async_copy(w[k], whole[k].at[:, bit["x"], bit["y"], bit["z"], bit["c"]], own_sem.at[k])

    def region(k, j, bits):
        h = heights[k]
        where = tuple(bits.get(a, slice(None)) for a in "xyz")
        return whole[k].at[(j // CHUNKS, *where, bit["c"], pl.ds((j % CHUNKS) * h, h))]

    def hop(k, stage, j):
        axes = ORDERS[k][: 3 - stage]
        part = region(k, j, {a: bit[a] for a in axes})
        return send(part, part, (tx.at[stage, k, j], rx.at[stage, k, j]), peer[ORDERS[k][2 - stage]])

    def forward(k, stage, j):
        bits = {a: bit[a] for a in ORDERS[k][: 3 - stage]}
        axis = ORDERS[k][2 - stage]
        bits[axis] = 1 - bit[axis]
        part = region(k, j, bits)
        return send(part, part, (ftx.at[stage, k, j], frx.at[stage, k, j]), peer["c"])

    def own_forward(k):
        part = whole[k].at[:, bit["x"], bit["y"], bit["z"], bit["c"]]
        return send(part, part, (own_tx.at[k], own_rx.at[k]), peer["c"])

    for k in range(3):
        own_copy(k).start()
    greet(me)
    for k in range(3):
        own_copy(k).wait()

    def first(j, _):
        for k in range(3):
            hop(k, 0, j).start()
        return 0

    lax.fori_loop(0, JOBS, first, 0)
    for k in range(3):
        own_forward(k).start()

    def turn(s, _):
        for stage in range(3):
            @pl.when((s >= stage) & (s < JOBS + stage))
            def _():
                j = s - stage
                for k in range(3):
                    hop(k, stage, j).wait_recv()
                    if stage < 2:
                        hop(k, stage + 1, j).start()
                    forward(k, stage, j).start()
        return 0

    lax.fori_loop(0, JOBS + 2, turn, 0)

    def drain(j, _):
        for k in range(3):
            for stage in range(3):
                hop(k, stage, j).wait_send()
                forward(k, stage, j).wait()
        return 0

    lax.fori_loop(0, JOBS, drain, 0)
    for k in range(3):
        own_forward(k).wait()


def gather(blocks):
    shapes = [b.shape[1:] for b in blocks]
    sem = pltpu.SemaphoreType.DMA
    whole = pl.pallas_call(
        gather_kernel,
        out_shape=[space((LAYERS, 2, 2, 2, 2, *s), BF16) for s, space in zip(shapes, SPACES, strict=True)],
        in_specs=[pl.BlockSpec(memory_space=pltpu.HBM)] * 3,
        out_specs=[pl.BlockSpec(memory_space=space) for space in SPACES],
        scratch_shapes=[sem((3,))] * 3 + [sem((3, 3, JOBS))] * 4,
        compiler_params=pltpu.CompilerParams(collective_id=1, has_side_effects=True, vmem_limit_bytes=2**20),
        name="gather",
    )(*blocks)
    return [t.reshape(LAYERS, DEVICES * s[0], s[1]) for t, s in zip(whole, shapes, strict=True)]


def solution(mesh):
    def step(*arrays):
        terms, weights, m, v = (arrays[i : i + 3] for i in (0, 3, 6, 9))
        sums, squares = scatter([t[0] for t in terms])
        count = DEVICES * sum(g.size for g in sums)
        factor = jnp.minimum(1.0, 0.5 * lax.rsqrt(squares / count + 1e-30))
        gradients = [g.astype(F32) * factor for g in sums]
        me = lax.axis_index("dp")
        own = [lax.dynamic_slice_in_dim(w, me * one.shape[1], one.shape[1], 1).astype(jnp.float32) for w, one in zip(weights, m, strict=True)]
        new = [adamw(w, m, v, g) for w, m, v, g in zip(own, m, v, gradients, strict=True)]
        whole = gather([one[0] for one in new])
        return (*whole, *(one[1] for one in new), *(one[2] for one in new))

    all_of, cut = P(None, None, None), P(None, "dp", None)
    return jax.shard_map(
        step,
        mesh=mesh,
        in_specs=(P(("rep", "dp"), None, None, None),) * 3 + (all_of,) * 3 + (cut,) * 6,
        out_specs=(P("rep", None, None),) * 3 + (P("rep", "dp", None),) * 6,
        check_vma=False,
    )
```

```python
import functools

import jax
import jax.numpy as jnp
from jax import lax
from jax.experimental import pallas as pl
from jax.experimental.pallas import tpu as pltpu
from jax.sharding import PartitionSpec as P

MESH = pl.DeviceIdType.MESH
BF16, F32 = jnp.bfloat16, jnp.float32
DEVICES = 16
LAYERS = 2
CUTS = ((4, 2), (4, 2), (8, 1))
CHUNKS = 8
JOBS = LAYERS * CHUNKS
SLOTS, AHEAD = 6, 2
GATHER_CHUNKS = 4
GATHER_JOBS = LAYERS * GATHER_CHUNKS
SCATTER_VMEM = 36
ORDERS = ("xyz", "yzx", "zxy")
STEP = {"x": 8, "y": 4, "z": 2, "c": 1}


def adamw(w, m, v, g):
    m = 0.9 * m + 0.1 * g
    v = 0.95 * v + 0.05 * g * g
    step = m * lax.rsqrt(v + 1e-8) + 0.1 * w
    return (w - 0.02 * step).astype(jnp.bfloat16), m, v


def place(me):
    bit = {a: (me // s) % 2 for a, s in STEP.items()}
    peer = {a: me + s - 2 * s * bit[a] for a, s in STEP.items()}
    return bit, peer


def greet(me):
    barrier = pltpu.get_barrier_semaphore()
    for i in range(1, DEVICES):
        pl.semaphore_signal(barrier, inc=1, device_id={"dp": (me + i) % DEVICES}, device_id_type=MESH)
    pl.semaphore_wait(barrier, DEVICES - 1)


def send(src, dst, sems, to):
    return pltpu.make_async_remote_copy(src, dst, sems[0], sems[1], device_id={"dp": to}, device_id_type=MESH)


def at_axis(ref, lead, axes, axis, bit):
    where = tuple(bit if a == axis else slice(None) for a in axes)
    return ref.at[(*lead, *where)]


def scatter_kernel(*refs):
    g, w, moments, refs = refs[:3], refs[3:6], refs[6:12], refs[12:]
    gb, total, own_w, held, refs = refs[:3], refs[3], refs[4:7], refs[7:13], refs[13:]
    own, s0, r1, r2, r3, acc = (refs[3 * i : 3 * i + 3] for i in range(6))
    mine, all_sq, own_sem, tx, rx, sq_tx, sq_rx, held_sem, free = refs[18:]
    me = lax.axis_index("dp")
    bit, peer = place(me)

    def piece(k, j):
        (h, w), n = r3[k].shape[-2:], CUTS[k][1]
        c = j % CHUNKS
        return j // CHUNKS, pl.ds((c // n) * h, h), pl.ds(pl.multiple_of((c % n) * w, w), w)

    def own_copy(k, j):
        layer, rows, cols = piece(k, j)
        return pltpu.make_async_copy(g[k].at[layer, :, :, :, bit["c"], rows, cols], own[k].at[j % 3], own_sem.at[k, j])

    def hop(k, stage, j):
        sems = (tx.at[stage, k, j], rx.at[stage, k, j])
        a1, a2, a3 = ORDERS[k]
        if stage == 0:
            layer, rows, cols = piece(k, j)
            return send(g[k].at[layer, :, :, :, 1 - bit["c"], rows, cols], s0[k].at[j % SLOTS], sems, peer["c"])
        if stage == 1:
            return send(at_axis(s0[k], (j % SLOTS,), "xyz", a1, 1 - bit[a1]), r1[k].at[j], sems, peer[a1])
        if stage == 2:
            rest = [a for a in "xyz" if a != a1]
            return send(at_axis(r1[k], (j,), rest, a2, 1 - bit[a2]), r2[k].at[j], sems, peer[a2])
        return send(r2[k].at[j, 1 - bit[a3]], r3[k].at[j], sems, peer[a3])

    def plus(a, b):
        return (a.astype(F32) + b.astype(F32)).astype(BF16)

    def fetch(j):
        for k in range(3):
            own_copy(k, j).start()
            hop(k, 0, j).start()

    staged = [pltpu.make_async_copy(w[k].at[:, bit["x"], bit["y"], bit["z"], bit["c"]], own_w[k], held_sem.at[k]) for k in range(3)]
    staged += [pltpu.make_async_copy(moments[i], held[i], held_sem.at[3 + i]) for i in range(6)]

    greet(me)
    for j in range(AHEAD):
        fetch(j)
    for one in staged:
        one.start()
    for k in range(3):
        acc[k][...] = jnp.zeros_like(acc[k])

    def turn(s, _):
        @pl.when((s >= SLOTS - AHEAD) & (s < JOBS - AHEAD))
        def _():
            pl.semaphore_wait(free, 1)

        @pl.when(s < JOBS - AHEAD)
        def _():
            fetch(s + AHEAD)

        @pl.when(s < JOBS)
        def _():
            for k in range(3):
                own_copy(k, s).wait()
                hop(k, 0, s).wait_recv()

                @pl.loop(0, 8)
                def _(b):
                    i = (b // 4, (b // 2) % 2, b % 2)
                    s0[k][(s % SLOTS, *i)] = plus(own[k][(s % 3, *i)], s0[k][(s % SLOTS, *i)])

                hop(k, 1, s).start()

        @pl.when((s >= 1) & (s < JOBS + 1))
        def _():
            j = s - 1
            for k in range(3):
                a1 = ORDERS[k][0]
                hop(k, 1, j).wait_recv()

                @pl.loop(0, 4)
                def _(b):
                    i = [b // 2, b % 2]
                    full = list(i)
                    full.insert("xyz".index(a1), bit[a1])
                    r1[k][(j, *i)] = plus(s0[k][(j % SLOTS, *full)], r1[k][(j, *i)])

                hop(k, 2, j).start()
            for k in range(3):
                hop(k, 1, j).wait_send()

            @pl.when(j < JOBS - SLOTS)
            def _():
                pl.semaphore_signal(free, inc=1, device_id={"dp": peer["c"]}, device_id_type=MESH)

        @pl.when((s >= 2) & (s < JOBS + 2))
        def _():
            j = s - 2
            for k in range(3):
                a1, a2, _a3 = ORDERS[k]
                rest = [a for a in "xyz" if a != a1]
                hop(k, 2, j).wait_recv()

                @pl.loop(0, 2)
                def _(b):
                    full = [b]
                    full.insert(rest.index(a2), bit[a2])
                    r2[k][j, b] = plus(r1[k][(j, *full)], r2[k][j, b])

                hop(k, 3, j).start()

        @pl.when(s >= 3)
        def _():
            j = s - 3
            for k in range(3):
                a3 = ORDERS[k][2]
                hop(k, 3, j).wait_recv()
                done = plus(r2[k][j, bit[a3]], r3[k][j])
                gb[k][piece(k, j)] = done
                wide = done.astype(F32)
                squares = wide * wide
                acc[k][...] += sum(squares[8 * i : 8 * i + 8] for i in range(done.shape[0] // 8))

        return 0

    lax.fori_loop(0, JOBS + 3, turn, 0)

    part = jnp.zeros((8, 128), F32)
    for k in range(3):
        a = acc[k][...]
        part += sum(a[:, 128 * i : 128 * i + 128] for i in range(a.shape[1] // 128))
    mine[...] = part
    all_sq[me] = part
    sends = [send(mine, all_sq.at[me], (sq_tx.at[i], sq_rx.at[i]), (me + i) % DEVICES) for i in range(1, DEVICES)]
    for one in sends:
        one.start()

    def drain(j, _):
        for k in range(3):
            for stage in (0, 2, 3):
                hop(k, stage, j).wait_send()
        return 0

    lax.fori_loop(0, JOBS, drain, 0)
    for one in staged:
        one.wait()
    for one in sends:
        one.wait()
    total[...] = jnp.full((8, 128), jnp.sum(sum(all_sq[i] for i in range(DEVICES))), F32)


def scatter(terms, weights, moments):
    blocks = [(t.shape[1] // DEVICES, t.shape[2]) for t in terms]
    split = [t.reshape(LAYERS, 2, 2, 2, 2, *b) for t, b in zip((*terms, *weights), (*blocks, *blocks), strict=True)]
    pieces = [(r // m, c // n) for (r, c), (m, n) in zip(blocks, CUTS, strict=True)]
    sem = pltpu.SemaphoreType.DMA
    leads = ((3, 2, 2, 2), (SLOTS, 2, 2, 2), (JOBS, 2, 2), (JOBS, 2), (JOBS,))
    scratch = [pltpu.VMEM((*lead, *p), BF16) for lead in leads for p in pieces]
    scratch += [pltpu.VMEM((8, c), F32) for _, c in pieces]
    scratch += [pltpu.VMEM((8, 128), F32), pltpu.VMEM((DEVICES, 8, 128), F32)]
    scratch += [sem((3, JOBS)), sem((4, 3, JOBS)), sem((4, 3, JOBS)), sem((DEVICES,)), sem((DEVICES,)), sem((9,)), pltpu.SemaphoreType.REGULAR]
    sums_0, sums_1, sums_2, total, *held = pl.pallas_call(
        scatter_kernel,
        out_shape=[pltpu.VMEM((LAYERS, *b), BF16) for b in blocks] + [pltpu.VMEM((8, 128), F32)] + [pltpu.VMEM((LAYERS, *b), BF16) for b in blocks] + [pltpu.VMEM(m.shape, F32) for m in moments],
        in_specs=[pl.BlockSpec(memory_space=pltpu.HBM)] * 12,
        out_specs=[pl.BlockSpec(memory_space=pltpu.VMEM)] * 13,
        scratch_shapes=scratch,
        compiler_params=pltpu.CompilerParams(collective_id=0, has_side_effects=True, vmem_limit_bytes=SCATTER_VMEM * 2**20),
        name="scatter",
    )(*split, *moments)
    return (sums_0, sums_1, sums_2), total[0, 0], held[:3], held[3:6], held[6:]


def gather_kernel(*refs):
    w, refs = refs[:3], refs[3:]
    whole, (own_tx, own_rx, tx, rx, ftx, frx) = refs[:3], refs[3:]
    me = lax.axis_index("dp")
    bit, peer = place(me)
    heights = [r.shape[-2] // GATHER_CHUNKS for r in whole]

    def region(k, j, bits):
        h = heights[k]
        where = tuple(bits.get(a, slice(None)) for a in "xyz")
        return whole[k].at[(j // GATHER_CHUNKS, *where, bit["c"], pl.ds((j % GATHER_CHUNKS) * h, h))]

    def hop(k, stage, j):
        axes = ORDERS[k][: 3 - stage]
        part = region(k, j, {a: bit[a] for a in axes})
        if stage == 0:
            h = heights[k]
            source = w[k].at[j // GATHER_CHUNKS, pl.ds((j % GATHER_CHUNKS) * h, h)]
        else:
            source = part
        return send(source, part, (tx.at[stage, k, j], rx.at[stage, k, j]), peer[ORDERS[k][2 - stage]])

    def forward(k, stage, j):
        bits = {a: bit[a] for a in ORDERS[k][: 3 - stage]}
        axis = ORDERS[k][2 - stage]
        bits[axis] = 1 - bit[axis]
        part = region(k, j, bits)
        return send(part, part, (ftx.at[stage, k, j], frx.at[stage, k, j]), peer["c"])

    def own_forward(k):
        part = whole[k].at[:, bit["x"], bit["y"], bit["z"], bit["c"]]
        return send(w[k], part, (own_tx.at[k], own_rx.at[k]), peer["c"])

    greet(me)

    def first(j, _):
        for k in range(3):
            hop(k, 0, j).start()
        return 0

    lax.fori_loop(0, GATHER_JOBS, first, 0)
    for k in range(3):
        own_forward(k).start()
    for k in range(3):
        whole[k][:, bit["x"], bit["y"], bit["z"], bit["c"]] = w[k][...]

    def turn(s, _):
        for stage in range(3):
            @pl.when((s >= stage) & (s < GATHER_JOBS + stage))
            def _():
                j = s - stage
                for k in range(3):
                    hop(k, stage, j).wait_recv()
                    if stage < 2:
                        hop(k, stage + 1, j).start()
                    forward(k, stage, j).start()
        return 0

    lax.fori_loop(0, GATHER_JOBS + 2, turn, 0)

    def drain(j, _):
        for k in range(3):
            for stage in range(3):
                hop(k, stage, j).wait_send()
                forward(k, stage, j).wait()
        return 0

    lax.fori_loop(0, GATHER_JOBS, drain, 0)
    for k in range(3):
        own_forward(k).wait()


def land_kernel(held, out, sem):
    one = pltpu.make_async_copy(held, out, sem)
    one.start()
    one.wait()


def gather(blocks):
    shapes = [b.shape[1:] for b in blocks]
    sem = pltpu.SemaphoreType.DMA
    whole = pl.pallas_call(
        gather_kernel,
        out_shape=[pltpu.VMEM((LAYERS, 2, 2, 2, 2, *s), BF16) for s in shapes],
        in_specs=[pl.BlockSpec(memory_space=pltpu.VMEM)] * 3,
        out_specs=[pl.BlockSpec(memory_space=pltpu.VMEM)] * 3,
        scratch_shapes=[sem((3,))] * 2 + [sem((3, 3, GATHER_JOBS))] * 4,
        compiler_params=pltpu.CompilerParams(collective_id=1, has_side_effects=True, vmem_limit_bytes=2**20),
        name="gather",
    )(*blocks)
    landed = [
        pl.pallas_call(
            land_kernel,
            out_shape=jax.ShapeDtypeStruct(t.shape, BF16),
            in_specs=[pl.BlockSpec(memory_space=pl.ANY)],
            out_specs=pl.BlockSpec(memory_space=pltpu.HBM),
            scratch_shapes=[sem],
            compiler_params=pltpu.CompilerParams(vmem_limit_bytes=2**19),
            name="land",
        )(t)
        for t in whole
    ]
    return [t.reshape(LAYERS, DEVICES * s[0], s[1]) for t, s in zip(landed, shapes, strict=True)]


def solution(mesh):
    def step(*arrays):
        terms, weights, m, v = (arrays[i : i + 3] for i in (0, 3, 6, 9))
        sums, squares, own, m, v = scatter([t[0] for t in terms], weights, (*m, *v))
        count = DEVICES * sum(g.size for g in sums)
        factor = jnp.minimum(1.0, 0.5 * lax.rsqrt(squares / count + 1e-30))
        gradients = [g.astype(F32) * factor for g in sums]
        new = [adamw(w.astype(F32), m, v, g) for w, m, v, g in zip(own, m, v, gradients, strict=True)]
        whole = gather([one[0] for one in new])
        return (*whole, *(one[1] for one in new), *(one[2] for one in new))

    all_of, cut = P(None, None, None), P(None, "dp", None)
    return jax.shard_map(
        step,
        mesh=mesh,
        in_specs=(P(("rep", "dp"), None, None, None),) * 3 + (all_of,) * 3 + (cut,) * 6,
        out_specs=(P("rep", None, None),) * 3 + (P("rep", "dp", None),) * 6,
        check_vma=False,
    )
```

```python
import functools

import jax
import jax.numpy as jnp
from jax import lax
from jax.experimental import pallas as pl
from jax.experimental.pallas import tpu as pltpu
from jax.sharding import PartitionSpec as P

MESH = pl.DeviceIdType.MESH
BF16, F32 = jnp.bfloat16, jnp.float32
DEVICES = 16
LAYERS = 2
CHUNKS = 4
JOBS = LAYERS * CHUNKS
FINE = 4
ITEMS = JOBS - 1 + FINE
SLOTS, AHEAD = 5, 3
LAGS = (1, 3, 5)
GATHER_CHUNKS = 4
GATHER_TAIL = 4
GATHER_JOBS = LAYERS * GATHER_CHUNKS
SCATTER_VMEM = 43
UPDATE_COLS, UPDATE_PARTS = 4096, 2
ORDERS = ("xyz", "yzx", "zxy")
STEP = {"x": 8, "y": 4, "z": 2, "c": 1}


def adamw(w, m, v, g):
    m = 0.9 * m + 0.1 * g
    v = 0.95 * v + 0.05 * g * g
    step = m * lax.rsqrt(v + 1e-8) + 0.1 * w
    return (w - 0.02 * step).astype(jnp.bfloat16), m, v


def place(me):
    bit = {a: (me // s) % 2 for a, s in STEP.items()}
    peer = {a: me + s - 2 * s * bit[a] for a, s in STEP.items()}
    return bit, peer


def greet_near(peer):
    barrier = pltpu.get_barrier_semaphore()
    for one in peer.values():
        pl.semaphore_signal(barrier, inc=1, device_id={"dp": one}, device_id_type=MESH)
    pl.semaphore_wait(barrier, len(peer))


def send(src, dst, sems, to):
    return pltpu.make_async_remote_copy(src, dst, sems[0], sems[1], device_id={"dp": to}, device_id_type=MESH)


def at_axis(ref, lead, axes, axis, bit):
    where = tuple(bit if a == axis else slice(None) for a in axes)
    return ref.at[(*lead, *where)]


def scatter_kernel(*refs):
    g, w, moments, refs = refs[:3], refs[3:6], refs[6:12], refs[12:]
    gb, total, own_w, held, refs = refs[:3], refs[3], refs[4:7], refs[7:13], refs[13:]
    own, s0, r1, r2, r3, acc = (refs[3 * i : 3 * i + 3] for i in range(6))
    mine, all_sq, own_sem, tx, rx, sq_tx, sq_rx, held_sem, free = refs[18:]
    me = lax.axis_index("dp")
    bit, peer = place(me)

    class Item:
        def __init__(self, i, fine):
            self.i, self.fine = i, fine
            self.j = 0 if fine else i - FINE + 1

        def part(self, k):
            h, w = r3[k].shape[-2:]
            if not self.fine:
                return pl.ds(0, h), pl.ds(0, w)
            if k == 2:
                return pl.ds(self.i * (h // FINE), h // FINE), pl.ds(0, w)
            return pl.ds(0, h), pl.ds(pl.multiple_of(self.i * (w // FINE), w // FINE), w // FINE)

        def piece(self, k):
            h = r3[k].shape[-2]
            rows, cols = self.part(k)
            return self.j // CHUNKS, pl.ds((self.j % CHUNKS) * h + rows.start, rows.size), cols

        def at(self, k, ref, lead, *where):
            return ref.at[(lead, *where, *self.part(k))]

        def own_copy(self, k):
            layer, rows, cols = self.piece(k)
            mine = self.at(k, own[k], self.i % 2, *[slice(None)] * 3)
            return pltpu.make_async_copy(g[k].at[layer, :, :, :, bit["c"], rows, cols], mine, own_sem.at[k, self.i])

        def hop(self, k, stage):
            sems = (tx.at[stage, k, self.i], rx.at[stage, k, self.i])
            a1, a2, a3 = ORDERS[k]
            every = slice(None)
            if stage == 0:
                layer, rows, cols = self.piece(k)
                theirs = self.at(k, s0[k], self.i % SLOTS, every, every, every)
                return send(g[k].at[layer, :, :, :, 1 - bit["c"], rows, cols], theirs, sems, peer["c"])
            if stage == 1:
                half = [1 - bit[a] if a == a1 else every for a in "xyz"]
                return send(self.at(k, s0[k], self.i % SLOTS, *half), self.at(k, r1[k], self.j, every, every), sems, peer[a1])
            if stage == 2:
                half = [1 - bit[a] if a == a2 else every for a in "xyz" if a != a1]
                return send(self.at(k, r1[k], self.j, *half), self.at(k, r2[k], self.j, every), sems, peer[a2])
            return send(self.at(k, r2[k], self.j, 1 - bit[a3]), self.at(k, r3[k], self.j), sems, peer[a3])

        def fetch(self):
            for k in range(3):
                self.own_copy(k).start()

        def cross(self):
            for k in range(3):
                self.hop(k, 0).start()

        def add_core(self):
            for k in range(3):
                self.own_copy(k).wait()
                self.hop(k, 0).wait_recv()

                @pl.loop(0, 2 if self.fine else 8)
                def _(b):
                    at = (b, slice(None), slice(None)) if self.fine else (b // 4, (b // 2) % 2, b % 2)
                    at = (*at, *self.part(k))
                    slot = (self.i % SLOTS, *at)
                    s0[k][slot] = plus(own[k][(self.i % 2, *at)], s0[k][slot])

                self.hop(k, 1).start()

        def add_first(self):
            for k in range(3):
                a1 = ORDERS[k][0]
                self.hop(k, 1).wait_recv()

                @pl.loop(0, 2 if self.fine else 4)
                def _(b):
                    at = [b, slice(None)] if self.fine else [b // 2, b % 2]
                    full = list(at)
                    full.insert("xyz".index(a1), bit[a1])
                    to = (self.j, *at, *self.part(k))
                    r1[k][to] = plus(s0[k][(self.i % SLOTS, *full, *self.part(k))], r1[k][to])

                self.hop(k, 2).start()
            for k in range(3):
                self.hop(k, 1).wait_send()

        def add_second(self):
            for k in range(3):
                a1, a2, _a3 = ORDERS[k]
                rest = [a for a in "xyz" if a != a1]
                self.hop(k, 2).wait_recv()

                @pl.loop(0, 2)
                def _(b):
                    full = [b]
                    full.insert(rest.index(a2), bit[a2])
                    to = (self.j, b, *self.part(k))
                    r2[k][to] = plus(r1[k][(self.j, *full, *self.part(k))], r2[k][to])

                self.hop(k, 3).start()

        def add_third(self):
            for k in range(3):
                self.hop(k, 3).wait_recv()
                done = plus(r2[k][(self.j, bit[ORDERS[k][2]], *self.part(k))], r3[k][(self.j, *self.part(k))])
                gb[k][self.piece(k)] = done
                wide = done.astype(F32)
                squares = wide * wide
                low = sum(squares[8 * i : 8 * i + 8] for i in range(done.shape[0] // 8))
                acc[k][...] += sum(low[:, 128 * i : 128 * i + 128] for i in range(low.shape[1] // 128))

        def drain(self):
            for k in range(3):
                for stage in (0, 2, 3):
                    self.hop(k, stage).wait_send()

    def plus(a, b):
        return (a.astype(F32) + b.astype(F32)).astype(BF16)

    def do(i, what):
        @pl.when((i >= 0) & (i < FINE))
        def _():
            getattr(Item(i, True), what)()

        @pl.when((i >= FINE) & (i < ITEMS))
        def _():
            getattr(Item(i, False), what)()

    staged = [pltpu.make_async_copy(w[k].at[:, bit["x"], bit["y"], bit["z"], bit["c"]], own_w[k], held_sem.at[k]) for k in range(3)]
    staged += [pltpu.make_async_copy(moments[i], held[i], held_sem.at[3 + i]) for i in range(6)]

    Item(0, True).fetch()
    greet_near(peer)
    for i in range(AHEAD):
        Item(i, True).cross()
    for k in range(3):
        acc[k][...] = jnp.zeros_like(acc[k])

    def turn(s, _):
        @pl.when((s >= SLOTS - AHEAD) & (s < ITEMS - AHEAD))
        def _():
            pl.semaphore_wait(free, 1)

        do(s + AHEAD, "cross")
        do(s + 1, "fetch")

        @pl.when(s == FINE)
        def _():
            for one in staged:
                one.start()

        do(s, "add_core")
        do(s - LAGS[0], "add_first")

        @pl.when((s >= LAGS[0]) & (s < LAGS[0] + ITEMS - SLOTS))
        def _():
            pl.semaphore_signal(free, inc=1, device_id={"dp": peer["c"]}, device_id_type=MESH)

        do(s - LAGS[1], "add_second")
        do(s - LAGS[2], "add_third")
        return 0

    lax.fori_loop(0, ITEMS + LAGS[2], turn, 0)

    part = jnp.zeros((8, 128), F32)
    for k in range(3):
        part += acc[k][...]
    part = jnp.sum(part, axis=0, keepdims=True)
    mine[...] = part
    all_sq[me] = part
    sends = [send(mine, all_sq.at[me], (sq_tx.at[i], sq_rx.at[i]), (me + i) % DEVICES) for i in range(1, DEVICES)]
    for one in sends:
        one.start()

    def drain(i, _):
        do(i, "drain")
        return 0

    lax.fori_loop(0, ITEMS, drain, 0)
    for one in staged:
        one.wait()
    for one in sends:
        one.wait()
    total[...] = jnp.full((8, 128), jnp.sum(sum(all_sq[i] for i in range(DEVICES))), F32)


def scatter(terms, weights, moments):
    blocks = [(t.shape[1] // DEVICES, t.shape[2]) for t in terms]
    split = [t.reshape(LAYERS, 2, 2, 2, 2, *b) for t, b in zip((*terms, *weights), (*blocks, *blocks), strict=True)]
    pieces = [(r // CHUNKS, c) for r, c in blocks]
    sem = pltpu.SemaphoreType.DMA
    leads = ((2, 2, 2, 2), (SLOTS, 2, 2, 2), (JOBS, 2, 2), (JOBS, 2), (JOBS,))
    scratch = [pltpu.VMEM((*lead, *p), BF16) for lead in leads for p in pieces]
    scratch += [pltpu.VMEM((8, 128), F32)] * 3
    scratch += [pltpu.VMEM((1, 128), F32), pltpu.VMEM((DEVICES, 1, 128), F32)]
    scratch += [sem((3, ITEMS)), sem((4, 3, ITEMS)), sem((4, 3, ITEMS)), sem((DEVICES,)), sem((DEVICES,)), sem((9,)), pltpu.SemaphoreType.REGULAR]
    sums_0, sums_1, sums_2, total, *held = pl.pallas_call(
        scatter_kernel,
        out_shape=[pltpu.VMEM((LAYERS, *b), BF16) for b in blocks] + [pltpu.VMEM((8, 128), F32)] + [pltpu.VMEM((LAYERS, *b), BF16) for b in blocks] + [pltpu.VMEM(m.shape, F32) for m in moments],
        in_specs=[pl.BlockSpec(memory_space=pltpu.HBM)] * 12,
        out_specs=[pl.BlockSpec(memory_space=pltpu.VMEM)] * 13,
        scratch_shapes=scratch,
        compiler_params=pltpu.CompilerParams(collective_id=0, has_side_effects=True, vmem_limit_bytes=SCATTER_VMEM * 2**20),
        name="scatter",
    )(*split, *moments)
    return (sums_0, sums_1, sums_2), total, held[:3], held[3:6], held[6:]


def update_kernel(*refs):
    g, w, m, v, total = refs[:3], refs[3:6], refs[6:9], refs[9:12], refs[12]
    new_w, out_m, out_v, refs = refs[13:16], refs[16:19], refs[19:22], refs[22:]
    new_m, new_v, sem = refs[:3], refs[3:6], refs[6]
    count = DEVICES * sum(LAYERS * r.shape[1] * r.shape[2] for r in g)
    factor = jnp.minimum(1.0, 0.5 * lax.rsqrt(total[...] / count + 1e-30))[:1, :1]
    copies = []
    for k in range(3):
        rows = 16 * UPDATE_COLS // g[k].shape[2]
        steps = g[k].shape[1] // rows

        for layer in range(LAYERS):
            for half in range(UPDATE_PARTS):
                part = steps // UPDATE_PARTS

                @pl.loop(half * part, (half + 1) * part)
                def _(i):
                    at = (layer, pl.ds(pl.multiple_of(i * rows, rows), rows))
                    new_w[k][at], new_m[k][at], new_v[k][at] = adamw(w[k][at].astype(F32), m[k][at], v[k][at], g[k][at].astype(F32) * factor)

                done = (layer, pl.ds(half * part * rows, part * rows))
                for new, out in ((new_m[k], out_m[k]), (new_v[k], out_v[k])):
                    copies.append(pltpu.make_async_copy(new.at[done], out.at[done], sem.at[len(copies)]))
                    copies[-1].start()
    for one in copies:
        one.wait()


def update(g, w, m, v, total):
    moments = [jax.ShapeDtypeStruct(one.shape, F32) for one in (*m, *v)]
    out = pl.pallas_call(
        update_kernel,
        out_shape=[pltpu.VMEM(one.shape, BF16) for one in w] + moments,
        in_specs=[pl.BlockSpec(memory_space=pltpu.VMEM)] * 13,
        out_specs=[pl.BlockSpec(memory_space=pltpu.VMEM)] * 3 + [pl.BlockSpec(memory_space=pltpu.HBM)] * 6,
        scratch_shapes=[pltpu.VMEM(one.shape, F32) for one in moments] + [pltpu.SemaphoreType.DMA((6 * LAYERS * UPDATE_PARTS,))],
        compiler_params=pltpu.CompilerParams(vmem_limit_bytes=14 * 2**20),
        name="update",
    )(*g, *w, *m, *v, total)
    return out[:3], out[3:6], out[6:]


def gather_kernel(*refs):
    w, refs = refs[:3], refs[3:]
    whole, (own_tx, own_rx, tx, rx, ftx, frx, last_tx, last_rx) = refs[:3], refs[3:]
    me = lax.axis_index("dp")
    bit, peer = place(me)
    heights = [r.shape[-2] // GATHER_CHUNKS for r in whole]

    def region(k, j, bits):
        h = heights[k]
        where = tuple(bits.get(a, slice(None)) for a in "xyz")
        return whole[k].at[(j // GATHER_CHUNKS, *where, bit["c"], pl.ds((j % GATHER_CHUNKS) * h, h))]

    def hop(k, stage, j):
        axes = ORDERS[k][: 3 - stage]
        part = region(k, j, {a: bit[a] for a in axes})
        if stage == 0:
            h = heights[k]
            source = w[k].at[j // GATHER_CHUNKS, pl.ds((j % GATHER_CHUNKS) * h, h)]
        else:
            source = part
        return send(source, part, (tx.at[stage, k, j], rx.at[stage, k, j]), peer[ORDERS[k][2 - stage]])

    def forward(k, stage, j):
        bits = {a: bit[a] for a in ORDERS[k][: 3 - stage]}
        axis = ORDERS[k][2 - stage]
        bits[axis] = 1 - bit[axis]
        part = region(k, j, bits)
        return send(part, part, (ftx.at[stage, k, j], frx.at[stage, k, j]), peer["c"])

    def last_hop(k, q, forward):
        axis = ORDERS[k][0]
        h = heights[k] // GATHER_TAIL if k == 2 else heights[k]
        w = whole[k].shape[-1] // (1 if k == 2 else GATHER_TAIL)
        row, col = (GATHER_CHUNKS - 1) * heights[k] + (q * h if k == 2 else 0), 0 if k == 2 else q * w
        where = tuple((1 - bit[axis] if forward else bit[axis]) if a == axis else slice(None) for a in "xyz")
        part = whole[k].at[(LAYERS - 1, *where, bit["c"], pl.ds(row, h), pl.ds(col, w))]
        way = int(forward)
        return send(part, part, (last_tx.at[way, k, q], last_rx.at[way, k, q]), peer["c" if forward else axis])

    def own_forward(k):
        part = whole[k].at[:, bit["x"], bit["y"], bit["z"], bit["c"]]
        return send(w[k], part, (own_tx.at[k], own_rx.at[k]), peer["c"])

    greet_near(peer)

    def first(j, _):
        for k in range(3):
            hop(k, 0, j).start()
        return 0

    lax.fori_loop(0, GATHER_JOBS, first, 0)
    for k in range(3):
        own_forward(k).start()
    for k in range(3):
        whole[k][:, bit["x"], bit["y"], bit["z"], bit["c"]] = w[k][...]

    def turn(s, _):
        for stage in range(3):
            end = GATHER_JOBS - 1 if stage == 2 else GATHER_JOBS

            @pl.when((s >= stage) & (s < end + stage))
            def _():
                j = s - stage
                for k in range(3):
                    hop(k, stage, j).wait_recv()
                    if stage == 0:
                        hop(k, 1, j).start()
                    if stage == 1:

                        @pl.when(j < GATHER_JOBS - 1)
                        def _():
                            hop(k, 2, j).start()

                        @pl.when(j == GATHER_JOBS - 1)
                        def _():
                            for q in range(GATHER_TAIL):
                                last_hop(k, q, False).start()

                    forward(k, stage, j).start()

        return 0

    lax.fori_loop(0, GATHER_JOBS + 1, turn, 0)
    for q in range(GATHER_TAIL):
        for k in range(3):
            last_hop(k, q, False).wait_recv()
            last_hop(k, q, True).start()

    def drain(j, _):
        for k in range(3):
            for stage in range(3):
                hop(k, stage, j).wait_send()
                forward(k, stage, j).wait()
        return 0

    lax.fori_loop(0, GATHER_JOBS - 1, drain, 0)
    for k in range(3):
        for stage in range(2):
            hop(k, stage, GATHER_JOBS - 1).wait_send()
            forward(k, stage, GATHER_JOBS - 1).wait()
        own_forward(k).wait()
        for q in range(GATHER_TAIL):
            last_hop(k, q, False).wait_send()
            last_hop(k, q, True).wait()


def land_kernel(held, out, sem):
    copies = [pltpu.make_async_copy(held.at[l, x], out.at[l, x], sem.at[2 * l + x]) for l in range(LAYERS) for x in range(2)]
    for one in copies:
        one.start()
    for one in copies:
        one.wait()


def gather(blocks):
    shapes = [b.shape[1:] for b in blocks]
    sem = pltpu.SemaphoreType.DMA
    whole = pl.pallas_call(
        gather_kernel,
        out_shape=[pltpu.VMEM((LAYERS, 2, 2, 2, 2, *s), BF16) for s in shapes],
        in_specs=[pl.BlockSpec(memory_space=pltpu.VMEM)] * 3,
        out_specs=[pl.BlockSpec(memory_space=pltpu.VMEM)] * 3,
        scratch_shapes=[sem((3,))] * 2 + [sem((3, 3, GATHER_JOBS))] * 4 + [sem((2, 3, GATHER_TAIL))] * 2,
        compiler_params=pltpu.CompilerParams(collective_id=1, has_side_effects=True, vmem_limit_bytes=2**20),
        name="gather",
    )(*blocks)
    landed = [
        pl.pallas_call(
            land_kernel,
            out_shape=jax.ShapeDtypeStruct(t.shape, BF16),
            in_specs=[pl.BlockSpec(memory_space=pl.ANY)],
            out_specs=pl.BlockSpec(memory_space=pltpu.HBM),
            scratch_shapes=[sem((4,))],
            compiler_params=pltpu.CompilerParams(vmem_limit_bytes=2**19),
            name="land",
        )(t)
        for t in whole
    ]
    return [t.reshape(LAYERS, DEVICES * s[0], s[1]) for t, s in zip(landed, shapes, strict=True)]


def solution(mesh):
    def step(*arrays):
        terms, weights, m, v = (arrays[i : i + 3] for i in (0, 3, 6, 9))
        sums, total, own, m, v = scatter([t[0] for t in terms], weights, (*m, *v))
        new, m, v = update(sums, own, m, v, total)
        whole = gather(new)
        return (*whole, *m, *v)

    all_of, cut = P(None, None, None), P(None, "dp", None)
    return jax.shard_map(
        step,
        mesh=mesh,
        in_specs=(P(("rep", "dp"), None, None, None),) * 3 + (all_of,) * 3 + (cut,) * 6,
        out_specs=(P("rep", None, None),) * 3 + (P("rep", "dp", None),) * 6,
        check_vma=False,
    )
```

```python
import functools

import jax
import jax.numpy as jnp
from jax import lax
from jax.experimental import pallas as pl
from jax.experimental.pallas import tpu as pltpu
from jax.sharding import PartitionSpec as P

MESH = pl.DeviceIdType.MESH
BF16, F32 = jnp.bfloat16, jnp.float32
DEVICES = 16
LAYERS = 2
CHUNKS = 4
JOBS = LAYERS * CHUNKS
FINE = 4
ITEMS = JOBS - 1 + FINE
SLOTS, AHEAD = 5, 3
LAGS = (1, 3, 5)
GATHER_CHUNKS = 2
GATHER_TAIL = 8
GATHER_JOBS = LAYERS * GATHER_CHUNKS
SCATTER_VMEM, LAND_VMEM = 44_700_000, 4 * 2**20
UPDATE_COLS, UPDATE_PARTS = 4096, 2
ORDERS = ("xyz", "yzx", "zxy")
STEP = {"x": 8, "y": 4, "z": 2, "c": 1}


def adamw(w, m, v, g):
    m = 0.9 * m + 0.1 * g
    v = 0.95 * v + 0.05 * g * g
    step = m * lax.rsqrt(v + 1e-8) + 0.1 * w
    return (w - 0.02 * step).astype(jnp.bfloat16), m, v


def place(me):
    bit = {a: (me // s) % 2 for a, s in STEP.items()}
    peer = {a: me + s - 2 * s * bit[a] for a, s in STEP.items()}
    return bit, peer


def greet_near(peer):
    barrier = pltpu.get_barrier_semaphore()
    for one in peer.values():
        pl.semaphore_signal(barrier, inc=1, device_id={"dp": one}, device_id_type=MESH)
    pl.semaphore_wait(barrier, len(peer))


def send(src, dst, sems, to):
    return pltpu.make_async_remote_copy(src, dst, sems[0], sems[1], device_id={"dp": to}, device_id_type=MESH)


def at_axis(ref, lead, axes, axis, bit):
    where = tuple(bit if a == axis else slice(None) for a in axes)
    return ref.at[(*lead, *where)]


def scatter_kernel(*refs):
    g, w, moments, refs = refs[:3], refs[3:6], refs[6:12], refs[12:]
    gb, total, own_w, held, refs = refs[:3], refs[3], refs[4:7], refs[7:13], refs[13:]
    own, s0, r1, r2, r3, acc = (refs[3 * i : 3 * i + 3] for i in range(6))
    mine, all_sq, own_sem, tx, rx, sq_tx, sq_rx, held_sem, free = refs[18:]
    me = lax.axis_index("dp")
    bit, peer = place(me)

    class Item:
        def __init__(self, i, fine):
            self.i, self.fine = i, fine
            self.j = 0 if fine else i - FINE + 1

        def part(self, k):
            h, w = r3[k].shape[-2:]
            if not self.fine:
                return pl.ds(0, h), pl.ds(0, w)
            if k == 2:
                return pl.ds(self.i * (h // FINE), h // FINE), pl.ds(0, w)
            return pl.ds(0, h), pl.ds(pl.multiple_of(self.i * (w // FINE), w // FINE), w // FINE)

        def piece(self, k):
            h = r3[k].shape[-2]
            rows, cols = self.part(k)
            return self.j // CHUNKS, pl.ds((self.j % CHUNKS) * h + rows.start, rows.size), cols

        def at(self, k, ref, lead, *where):
            return ref.at[(lead, *where, *self.part(k))]

        def own_copy(self, k):
            layer, rows, cols = self.piece(k)
            mine = self.at(k, own[k], self.i % 2, *[slice(None)] * 3)
            return pltpu.make_async_copy(g[k].at[layer, :, :, :, bit["c"], rows, cols], mine, own_sem.at[k, self.i])

        def hop(self, k, stage):
            sems = (tx.at[stage, k, self.i], rx.at[stage, k, self.i])
            a1, a2, a3 = ORDERS[k]
            every = slice(None)
            if stage == 0:
                layer, rows, cols = self.piece(k)
                theirs = self.at(k, s0[k], self.i % SLOTS, every, every, every)
                return send(g[k].at[layer, :, :, :, 1 - bit["c"], rows, cols], theirs, sems, peer["c"])
            if stage == 1:
                half = [1 - bit[a] if a == a1 else every for a in "xyz"]
                return send(self.at(k, s0[k], self.i % SLOTS, *half), self.at(k, r1[k], self.j, every, every), sems, peer[a1])
            if stage == 2:
                half = [1 - bit[a] if a == a2 else every for a in "xyz" if a != a1]
                return send(self.at(k, r1[k], self.j, *half), self.at(k, r2[k], self.j, every), sems, peer[a2])
            return send(self.at(k, r2[k], self.j, 1 - bit[a3]), self.at(k, r3[k], self.j), sems, peer[a3])

        def fetch(self):
            for k in range(3):
                self.own_copy(k).start()

        def cross(self):
            for k in range(3):
                self.hop(k, 0).start()

        def add_core(self):
            for k in range(3):
                self.own_copy(k).wait()
                self.hop(k, 0).wait_recv()

                @pl.loop(0, 2 if self.fine else 8)
                def _(b):
                    at = (b, slice(None), slice(None)) if self.fine else (b // 4, (b // 2) % 2, b % 2)
                    at = (*at, *self.part(k))
                    slot = (self.i % SLOTS, *at)
                    s0[k][slot] = plus(own[k][(self.i % 2, *at)], s0[k][slot])

                self.hop(k, 1).start()

        def add_first(self):
            for k in range(3):
                a1 = ORDERS[k][0]
                self.hop(k, 1).wait_recv()

                @pl.loop(0, 2 if self.fine else 4)
                def _(b):
                    at = [b, slice(None)] if self.fine else [b // 2, b % 2]
                    full = list(at)
                    full.insert("xyz".index(a1), bit[a1])
                    to = (self.j, *at, *self.part(k))
                    r1[k][to] = plus(s0[k][(self.i % SLOTS, *full, *self.part(k))], r1[k][to])

                self.hop(k, 2).start()
            for k in range(3):
                self.hop(k, 1).wait_send()

        def add_second(self):
            for k in range(3):
                a1, a2, _a3 = ORDERS[k]
                rest = [a for a in "xyz" if a != a1]
                self.hop(k, 2).wait_recv()

                @pl.loop(0, 2)
                def _(b):
                    full = [b]
                    full.insert(rest.index(a2), bit[a2])
                    to = (self.j, b, *self.part(k))
                    r2[k][to] = plus(r1[k][(self.j, *full, *self.part(k))], r2[k][to])

                self.hop(k, 3).start()

        def add_third(self):
            for k in range(3):
                self.hop(k, 3).wait_recv()
                done = plus(r2[k][(self.j, bit[ORDERS[k][2]], *self.part(k))], r3[k][(self.j, *self.part(k))])
                gb[k][self.piece(k)] = done
                wide = done.astype(F32)
                squares = wide * wide
                low = sum(squares[8 * i : 8 * i + 8] for i in range(done.shape[0] // 8))
                acc[k][...] += sum(low[:, 128 * i : 128 * i + 128] for i in range(low.shape[1] // 128))

        def drain(self):
            for k in range(3):
                for stage in (0, 2, 3):
                    self.hop(k, stage).wait_send()

    def plus(a, b):
        return (a.astype(F32) + b.astype(F32)).astype(BF16)

    def do(i, what):
        @pl.when((i >= 0) & (i < FINE))
        def _():
            getattr(Item(i, True), what)()

        @pl.when((i >= FINE) & (i < ITEMS))
        def _():
            getattr(Item(i, False), what)()

    staged = [pltpu.make_async_copy(w[k].at[:, bit["x"], bit["y"], bit["z"], bit["c"]], own_w[k], held_sem.at[k]) for k in range(3)]
    staged += [pltpu.make_async_copy(moments[i], held[i], held_sem.at[3 + i]) for i in range(6)]

    Item(0, True).fetch()
    greet_near(peer)
    for i in range(AHEAD):
        Item(i, True).cross()
    for k in range(3):
        acc[k][...] = jnp.zeros_like(acc[k])

    def turn(s, _):
        @pl.when((s >= SLOTS - AHEAD) & (s < ITEMS - AHEAD))
        def _():
            pl.semaphore_wait(free, 1)

        do(s + AHEAD, "cross")
        do(s + 1, "fetch")

        @pl.when(s == FINE)
        def _():
            for one in staged:
                one.start()

        do(s, "add_core")
        do(s - LAGS[0], "add_first")

        @pl.when((s >= LAGS[0]) & (s < LAGS[0] + ITEMS - SLOTS))
        def _():
            pl.semaphore_signal(free, inc=1, device_id={"dp": peer["c"]}, device_id_type=MESH)

        do(s - LAGS[1], "add_second")
        do(s - LAGS[2], "add_third")
        return 0

    lax.fori_loop(0, ITEMS + LAGS[2], turn, 0)

    part = jnp.zeros((8, 128), F32)
    for k in range(3):
        part += acc[k][...]
    part = jnp.sum(part, axis=0, keepdims=True)
    mine[...] = part
    all_sq[me] = part
    sends = [send(mine, all_sq.at[me], (sq_tx.at[i], sq_rx.at[i]), (me + i) % DEVICES) for i in range(1, DEVICES)]
    for one in sends:
        one.start()

    def drain(i, _):
        do(i, "drain")
        return 0

    lax.fori_loop(0, ITEMS, drain, 0)
    for one in staged:
        one.wait()
    for one in sends:
        one.wait()
    total[...] = jnp.full((8, 128), jnp.sum(sum(all_sq[i] for i in range(DEVICES))), F32)


def scatter(terms, weights, moments):
    blocks = [(t.shape[1] // DEVICES, t.shape[2]) for t in terms]
    split = [t.reshape(LAYERS, 2, 2, 2, 2, *b) for t, b in zip((*terms, *weights), (*blocks, *blocks), strict=True)]
    pieces = [(r // CHUNKS, c) for r, c in blocks]
    sem = pltpu.SemaphoreType.DMA
    leads = ((2, 2, 2, 2), (SLOTS, 2, 2, 2), (JOBS, 2, 2), (JOBS, 2), (JOBS,))
    scratch = [pltpu.VMEM((*lead, *p), BF16) for lead in leads for p in pieces]
    scratch += [pltpu.VMEM((8, 128), F32)] * 3
    scratch += [pltpu.VMEM((1, 128), F32), pltpu.VMEM((DEVICES, 1, 128), F32)]
    scratch += [sem((3, ITEMS)), sem((4, 3, ITEMS)), sem((4, 3, ITEMS)), sem((DEVICES,)), sem((DEVICES,)), sem((9,)), pltpu.SemaphoreType.REGULAR]
    sums_0, sums_1, sums_2, total, *held = pl.pallas_call(
        scatter_kernel,
        out_shape=[pltpu.VMEM((LAYERS, *b), BF16) for b in blocks] + [pltpu.VMEM((8, 128), F32)] + [pltpu.VMEM((LAYERS, *b), BF16) for b in blocks] + [pltpu.VMEM(m.shape, F32) for m in moments],
        in_specs=[pl.BlockSpec(memory_space=pltpu.HBM)] * 12,
        out_specs=[pl.BlockSpec(memory_space=pltpu.VMEM)] * 13,
        scratch_shapes=scratch,
        compiler_params=pltpu.CompilerParams(collective_id=0, has_side_effects=True, vmem_limit_bytes=SCATTER_VMEM),
        name="scatter",
    )(*split, *moments)
    return (sums_0, sums_1, sums_2), total, held[:3], held[3:6], held[6:]


def update_kernel(*refs):
    g, w, m, v, total = refs[:3], refs[3:6], refs[6:9], refs[9:12], refs[12]
    new_w, out_m, out_v, refs = refs[13:16], refs[16:19], refs[19:22], refs[22:]
    new_m, new_v, sem = refs[:3], refs[3:6], refs[6]
    count = DEVICES * sum(LAYERS * r.shape[1] * r.shape[2] for r in g)
    factor = jnp.minimum(1.0, 0.5 * lax.rsqrt(total[...] / count + 1e-30))[:1, :1]
    copies = []
    for k in range(3):
        rows = 16 * UPDATE_COLS // g[k].shape[2]
        steps = g[k].shape[1] // rows

        for layer in range(LAYERS):
            for half in range(UPDATE_PARTS):
                part = steps // UPDATE_PARTS

                @pl.loop(half * part, (half + 1) * part)
                def _(i):
                    at = (layer, pl.ds(pl.multiple_of(i * rows, rows), rows))
                    new_w[k][at], new_m[k][at], new_v[k][at] = adamw(w[k][at].astype(F32), m[k][at], v[k][at], g[k][at].astype(F32) * factor)

                done = (layer, pl.ds(half * part * rows, part * rows))
                for new, out in ((new_m[k], out_m[k]), (new_v[k], out_v[k])):
                    copies.append(pltpu.make_async_copy(new.at[done], out.at[done], sem.at[len(copies)]))
                    copies[-1].start()
    for one in copies:
        one.wait()


def update(g, w, m, v, total):
    moments = [jax.ShapeDtypeStruct(one.shape, F32) for one in (*m, *v)]
    out = pl.pallas_call(
        update_kernel,
        out_shape=[pltpu.VMEM(one.shape, BF16) for one in w] + moments,
        in_specs=[pl.BlockSpec(memory_space=pltpu.VMEM)] * 13,
        out_specs=[pl.BlockSpec(memory_space=pltpu.VMEM)] * 3 + [pl.BlockSpec(memory_space=pltpu.HBM)] * 6,
        scratch_shapes=[pltpu.VMEM(one.shape, F32) for one in moments] + [pltpu.SemaphoreType.DMA((6 * LAYERS * UPDATE_PARTS,))],
        compiler_params=pltpu.CompilerParams(vmem_limit_bytes=14 * 2**20),
        name="update",
    )(*g, *w, *m, *v, total)
    return out[:3], out[3:6], out[6:]


def gather_kernel(*refs):
    w, refs = refs[:3], refs[3:]
    whole, (own_tx, own_rx, tx, rx, ftx, frx, last_tx, last_rx) = refs[:3], refs[3:]
    me = lax.axis_index("dp")
    bit, peer = place(me)
    heights = [r.shape[-2] // GATHER_CHUNKS for r in whole]

    def region(k, j, bits):
        h = heights[k]
        where = tuple(bits.get(a, slice(None)) for a in "xyz")
        return whole[k].at[(j // GATHER_CHUNKS, *where, bit["c"], pl.ds((j % GATHER_CHUNKS) * h, h))]

    def hop(k, stage, j):
        axes = ORDERS[k][: 3 - stage]
        part = region(k, j, {a: bit[a] for a in axes})
        if stage == 0:
            h = heights[k]
            source = w[k].at[j // GATHER_CHUNKS, pl.ds((j % GATHER_CHUNKS) * h, h)]
        else:
            source = part
        return send(source, part, (tx.at[stage, k, j], rx.at[stage, k, j]), peer[ORDERS[k][2 - stage]])

    def forward(k, stage, j):
        bits = {a: bit[a] for a in ORDERS[k][: 3 - stage]}
        axis = ORDERS[k][2 - stage]
        bits[axis] = 1 - bit[axis]
        part = region(k, j, bits)
        return send(part, part, (ftx.at[stage, k, j], frx.at[stage, k, j]), peer["c"])

    def last_hop(k, q, forward):
        axis = ORDERS[k][0]
        h = heights[k] // GATHER_TAIL if k == 2 else heights[k]
        w = whole[k].shape[-1] // (1 if k == 2 else GATHER_TAIL)
        row, col = (GATHER_CHUNKS - 1) * heights[k] + (q * h if k == 2 else 0), 0 if k == 2 else q * w
        where = tuple((1 - bit[axis] if forward else bit[axis]) if a == axis else slice(None) for a in "xyz")
        part = whole[k].at[(LAYERS - 1, *where, bit["c"], pl.ds(row, h), pl.ds(col, w))]
        way = int(forward)
        return send(part, part, (last_tx.at[way, k, q], last_rx.at[way, k, q]), peer["c" if forward else axis])

    def own_forward(k):
        part = whole[k].at[:, bit["x"], bit["y"], bit["z"], bit["c"]]
        return send(w[k], part, (own_tx.at[k], own_rx.at[k]), peer["c"])

    greet_near(peer)

    def first(j, _):
        for k in range(3):
            hop(k, 0, j).start()
        return 0

    lax.fori_loop(0, GATHER_JOBS, first, 0)
    for k in range(3):
        own_forward(k).start()
    for k in range(3):
        whole[k][:, bit["x"], bit["y"], bit["z"], bit["c"]] = w[k][...]

    def turn(s, _):
        for stage in range(3):
            end = GATHER_JOBS - 1 if stage == 2 else GATHER_JOBS

            @pl.when((s >= stage) & (s < end + stage))
            def _():
                j = s - stage
                for k in range(3):
                    hop(k, stage, j).wait_recv()
                    if stage == 0:
                        hop(k, 1, j).start()
                    if stage == 1:

                        @pl.when(j < GATHER_JOBS - 1)
                        def _():
                            hop(k, 2, j).start()

                        @pl.when(j == GATHER_JOBS - 1)
                        def _():
                            for q in range(GATHER_TAIL):
                                last_hop(k, q, False).start()

                    forward(k, stage, j).start()

        return 0

    lax.fori_loop(0, GATHER_JOBS + 1, turn, 0)
    for q in range(GATHER_TAIL):
        for k in range(3):
            last_hop(k, q, False).wait_recv()
            last_hop(k, q, True).start()

    def drain(j, _):
        for k in range(3):
            for stage in range(3):
                hop(k, stage, j).wait_send()
                forward(k, stage, j).wait()
        return 0

    lax.fori_loop(0, GATHER_JOBS - 1, drain, 0)
    for k in range(3):
        for stage in range(2):
            hop(k, stage, GATHER_JOBS - 1).wait_send()
            forward(k, stage, GATHER_JOBS - 1).wait()
        own_forward(k).wait()
        for q in range(GATHER_TAIL):
            last_hop(k, q, False).wait_send()
            last_hop(k, q, True).wait()


def land_kernel(*refs):
    held, out, sem = refs[:3], refs[3:6], refs[6]
    copies = [pltpu.make_async_copy(held[k].at[l, x], out[k].at[l, x], sem.at[k, l, x]) for k in range(3) for l in range(LAYERS) for x in range(2)]
    for one in copies:
        one.start()
    for one in copies:
        one.wait()


def gather(blocks):
    shapes = [b.shape[1:] for b in blocks]
    sem = pltpu.SemaphoreType.DMA
    whole = pl.pallas_call(
        gather_kernel,
        out_shape=[pltpu.VMEM((LAYERS, 2, 2, 2, 2, *s), BF16) for s in shapes],
        in_specs=[pl.BlockSpec(memory_space=pltpu.VMEM)] * 3,
        out_specs=[pl.BlockSpec(memory_space=pltpu.VMEM)] * 3,
        scratch_shapes=[sem((3,))] * 2 + [sem((3, 3, GATHER_JOBS))] * 4 + [sem((2, 3, GATHER_TAIL))] * 2,
        compiler_params=pltpu.CompilerParams(collective_id=1, has_side_effects=True, vmem_limit_bytes=2**20),
        name="gather",
    )(*blocks)
    landed = pl.pallas_call(
        land_kernel,
        out_shape=[jax.ShapeDtypeStruct(one.shape, BF16) for one in whole],
        in_specs=[pl.BlockSpec(memory_space=pltpu.VMEM)] * 3,
        out_specs=[pl.BlockSpec(memory_space=pltpu.HBM)] * 3,
        scratch_shapes=[sem((3, LAYERS, 2))],
        compiler_params=pltpu.CompilerParams(vmem_limit_bytes=LAND_VMEM),
        name="land",
    )(*whole)
    return [t.reshape(LAYERS, DEVICES * s[0], s[1]) for t, s in zip(landed, shapes, strict=True)]


def solution(mesh):
    def step(*arrays):
        terms, weights, m, v = (arrays[i : i + 3] for i in (0, 3, 6, 9))
        sums, total, own, m, v = scatter([t[0] for t in terms], weights, (*m, *v))
        new, m, v = update(sums, own, m, v, total)
        whole = gather(new)
        return (*whole, *m, *v)

    all_of, cut = P(None, None, None), P(None, "dp", None)
    return jax.shard_map(
        step,
        mesh=mesh,
        in_specs=(P(("rep", "dp"), None, None, None),) * 3 + (all_of,) * 3 + (cut,) * 6,
        out_specs=(P("rep", None, None),) * 3 + (P("rep", "dp", None),) * 6,
        check_vma=False,
    )
```

```python
import functools

import jax
import jax.numpy as jnp
from jax import lax
from jax.experimental import pallas as pl
from jax.experimental.pallas import tpu as pltpu
from jax.sharding import PartitionSpec as P

MESH = pl.DeviceIdType.MESH
BF16, F32 = jnp.bfloat16, jnp.float32
DEVICES = 16
LAYERS = 2
CHUNKS = 4
JOBS = LAYERS * CHUNKS
FINE = 4
ITEMS = JOBS - 1 + FINE
SLOTS, AHEAD = 5, 3
LAGS = (1, 3, 5)
GATHER_CHUNKS = 1
GATHER_TAIL = 8
GATHER_JOBS = LAYERS * GATHER_CHUNKS
SCATTER_VMEM, LAND_VMEM = 44_700_000, 4 * 2**20
UPDATE_COLS, UPDATE_PARTS = 4096, 2
ORDERS = ("xyz", "yzx", "zxy")
STEP = {"x": 8, "y": 4, "z": 2, "c": 1}


def adamw(w, m, v, h):
    m = 0.9 * m + h
    v = 0.95 * v + (5.0 * h) * h
    return (0.998 * w - (0.02 * m) * lax.rsqrt(v + 1e-8)).astype(jnp.bfloat16), m, v


def place(me):
    bit = {a: (me // s) % 2 for a, s in STEP.items()}
    peer = {a: me + s - 2 * s * bit[a] for a, s in STEP.items()}
    return bit, peer


def greet_near(peer):
    barrier = pltpu.get_barrier_semaphore()
    for one in peer.values():
        pl.semaphore_signal(barrier, inc=1, device_id={"dp": one}, device_id_type=MESH)
    pl.semaphore_wait(barrier, len(peer))


def send(src, dst, sems, to):
    return pltpu.make_async_remote_copy(src, dst, sems[0], sems[1], device_id={"dp": to}, device_id_type=MESH)


def at_axis(ref, lead, axes, axis, bit):
    where = tuple(bit if a == axis else slice(None) for a in axes)
    return ref.at[(*lead, *where)]


def scatter_kernel(*refs):
    g, w, moments, refs = refs[:3], refs[3:6], refs[6:12], refs[12:]
    gb, total, own_w, held, refs = refs[:3], refs[3], refs[4:7], refs[7:13], refs[13:]
    own, s0, r1, r2, r3, acc = (refs[3 * i : 3 * i + 3] for i in range(6))
    mine, all_sq, own_sem, tx, rx, sq_tx, sq_rx, held_sem, free = refs[18:]
    me = lax.axis_index("dp")
    bit, peer = place(me)

    class Item:
        def __init__(self, i, fine):
            self.i, self.fine = i, fine
            self.j = 0 if fine else i - FINE + 1

        def part(self, k):
            h, w = r3[k].shape[-2:]
            if not self.fine:
                return pl.ds(0, h), pl.ds(0, w)
            if k == 2:
                return pl.ds(self.i * (h // FINE), h // FINE), pl.ds(0, w)
            return pl.ds(0, h), pl.ds(pl.multiple_of(self.i * (w // FINE), w // FINE), w // FINE)

        def piece(self, k):
            h = r3[k].shape[-2]
            rows, cols = self.part(k)
            return self.j // CHUNKS, pl.ds((self.j % CHUNKS) * h + rows.start, rows.size), cols

        def at(self, k, ref, lead, *where):
            return ref.at[(lead, *where, *self.part(k))]

        def own_copy(self, k):
            layer, rows, cols = self.piece(k)
            mine = self.at(k, own[k], self.i % 2, *[slice(None)] * 3)
            return pltpu.make_async_copy(g[k].at[layer, :, :, :, bit["c"], rows, cols], mine, own_sem.at[k, self.i])

        def hop(self, k, stage):
            sems = (tx.at[stage, k, self.i], rx.at[stage, k, self.i])
            a1, a2, a3 = ORDERS[k]
            every = slice(None)
            if stage == 0:
                layer, rows, cols = self.piece(k)
                theirs = self.at(k, s0[k], self.i % SLOTS, every, every, every)
                return send(g[k].at[layer, :, :, :, 1 - bit["c"], rows, cols], theirs, sems, peer["c"])
            if stage == 1:
                half = [1 - bit[a] if a == a1 else every for a in "xyz"]
                return send(self.at(k, s0[k], self.i % SLOTS, *half), self.at(k, r1[k], self.j, every, every), sems, peer[a1])
            if stage == 2:
                half = [1 - bit[a] if a == a2 else every for a in "xyz" if a != a1]
                return send(self.at(k, r1[k], self.j, *half), self.at(k, r2[k], self.j, every), sems, peer[a2])
            return send(self.at(k, r2[k], self.j, 1 - bit[a3]), self.at(k, r3[k], self.j), sems, peer[a3])

        def fetch(self):
            for k in range(3):
                self.own_copy(k).start()

        def cross(self):
            for k in range(3):
                self.hop(k, 0).start()

        def add_core(self):
            for k in range(3):
                self.own_copy(k).wait()
                self.hop(k, 0).wait_recv()

                @pl.loop(0, 2 if self.fine else 8)
                def _(b):
                    at = (b, slice(None), slice(None)) if self.fine else (b // 4, (b // 2) % 2, b % 2)
                    at = (*at, *self.part(k))
                    slot = (self.i % SLOTS, *at)
                    s0[k][slot] = plus(own[k][(self.i % 2, *at)], s0[k][slot])

                self.hop(k, 1).start()

        def add_first(self):
            for k in range(3):
                a1 = ORDERS[k][0]
                self.hop(k, 1).wait_recv()

                @pl.loop(0, 2 if self.fine else 4)
                def _(b):
                    at = [b, slice(None)] if self.fine else [b // 2, b % 2]
                    full = list(at)
                    full.insert("xyz".index(a1), bit[a1])
                    to = (self.j, *at, *self.part(k))
                    r1[k][to] = plus(s0[k][(self.i % SLOTS, *full, *self.part(k))], r1[k][to])

                self.hop(k, 2).start()
            for k in range(3):
                self.hop(k, 1).wait_send()

        def add_second(self):
            for k in range(3):
                a1, a2, _a3 = ORDERS[k]
                rest = [a for a in "xyz" if a != a1]
                self.hop(k, 2).wait_recv()

                @pl.loop(0, 2)
                def _(b):
                    full = [b]
                    full.insert(rest.index(a2), bit[a2])
                    to = (self.j, b, *self.part(k))
                    r2[k][to] = plus(r1[k][(self.j, *full, *self.part(k))], r2[k][to])

                self.hop(k, 3).start()

        def add_third(self):
            for k in range(3):
                self.hop(k, 3).wait_recv()
                done = plus(r2[k][(self.j, bit[ORDERS[k][2]], *self.part(k))], r3[k][(self.j, *self.part(k))])
                gb[k][self.piece(k)] = done
                wide = done.astype(F32)
                squares = wide * wide
                low = sum(squares[8 * i : 8 * i + 8] for i in range(done.shape[0] // 8))
                acc[k][...] += sum(low[:, 128 * i : 128 * i + 128] for i in range(low.shape[1] // 128))

        def drain(self):
            for k in range(3):
                for stage in (0, 2, 3):
                    self.hop(k, stage).wait_send()

    def plus(a, b):
        return (a.astype(F32) + b.astype(F32)).astype(BF16)

    def do(i, what):
        @pl.when((i >= 0) & (i < FINE))
        def _():
            getattr(Item(i, True), what)()

        @pl.when((i >= FINE) & (i < ITEMS))
        def _():
            getattr(Item(i, False), what)()

    staged = [pltpu.make_async_copy(w[k].at[:, bit["x"], bit["y"], bit["z"], bit["c"]], own_w[k], held_sem.at[k]) for k in range(3)]
    staged += [pltpu.make_async_copy(moments[i], held[i], held_sem.at[3 + i]) for i in range(6)]

    Item(0, True).fetch()
    greet_near(peer)
    for i in range(AHEAD):
        Item(i, True).cross()
    for k in range(3):
        acc[k][...] = jnp.zeros_like(acc[k])

    def turn(s, _):
        @pl.when((s >= SLOTS - AHEAD) & (s < ITEMS - AHEAD))
        def _():
            pl.semaphore_wait(free, 1)

        do(s + AHEAD, "cross")
        do(s + 1, "fetch")

        @pl.when(s == FINE)
        def _():
            for one in staged:
                one.start()

        do(s, "add_core")
        do(s - LAGS[0], "add_first")

        @pl.when((s >= LAGS[0]) & (s < LAGS[0] + ITEMS - SLOTS))
        def _():
            pl.semaphore_signal(free, inc=1, device_id={"dp": peer["c"]}, device_id_type=MESH)

        do(s - LAGS[1], "add_second")
        do(s - LAGS[2], "add_third")
        return 0

    lax.fori_loop(0, ITEMS + LAGS[2], turn, 0)

    part = jnp.zeros((8, 128), F32)
    for k in range(3):
        part += acc[k][...]
    part = jnp.sum(part, axis=0, keepdims=True)
    mine[...] = part
    all_sq[me] = part
    sends = [send(mine, all_sq.at[me], (sq_tx.at[i], sq_rx.at[i]), (me + i) % DEVICES) for i in range(1, DEVICES)]
    for one in sends:
        one.start()

    def drain(i, _):
        do(i, "drain")
        return 0

    lax.fori_loop(0, ITEMS, drain, 0)
    for one in staged:
        one.wait()
    for one in sends:
        one.wait()
    total[...] = jnp.full((8, 128), jnp.sum(sum(all_sq[i] for i in range(DEVICES))), F32)


def scatter(terms, weights, moments):
    blocks = [(t.shape[1] // DEVICES, t.shape[2]) for t in terms]
    split = [t.reshape(LAYERS, 2, 2, 2, 2, *b) for t, b in zip((*terms, *weights), (*blocks, *blocks), strict=True)]
    pieces = [(r // CHUNKS, c) for r, c in blocks]
    sem = pltpu.SemaphoreType.DMA
    leads = ((2, 2, 2, 2), (SLOTS, 2, 2, 2), (JOBS, 2, 2), (JOBS, 2), (JOBS,))
    scratch = [pltpu.VMEM((*lead, *p), BF16) for lead in leads for p in pieces]
    scratch += [pltpu.VMEM((8, 128), F32)] * 3
    scratch += [pltpu.VMEM((1, 128), F32), pltpu.VMEM((DEVICES, 1, 128), F32)]
    scratch += [sem((3, ITEMS)), sem((4, 3, ITEMS)), sem((4, 3, ITEMS)), sem((DEVICES,)), sem((DEVICES,)), sem((9,)), pltpu.SemaphoreType.REGULAR]
    sums_0, sums_1, sums_2, total, *held = pl.pallas_call(
        scatter_kernel,
        out_shape=[pltpu.VMEM((LAYERS, *b), BF16) for b in blocks] + [pltpu.VMEM((8, 128), F32)] + [pltpu.VMEM((LAYERS, *b), BF16) for b in blocks] + [pltpu.VMEM(m.shape, F32) for m in moments],
        in_specs=[pl.BlockSpec(memory_space=pltpu.HBM)] * 12,
        out_specs=[pl.BlockSpec(memory_space=pltpu.VMEM)] * 13,
        scratch_shapes=scratch,
        compiler_params=pltpu.CompilerParams(collective_id=0, has_side_effects=True, vmem_limit_bytes=SCATTER_VMEM),
        name="scatter",
    )(*split, *moments)
    return (sums_0, sums_1, sums_2), total, held[:3], held[3:6], held[6:]


def update_kernel(*refs):
    g, w, m, v, total = refs[:3], refs[3:6], refs[6:9], refs[9:12], refs[12]
    new_w, out_m, out_v, refs = refs[13:16], refs[16:19], refs[19:22], refs[22:]
    new_m, new_v, sem = refs[:3], refs[3:6], refs[6]
    count = DEVICES * sum(LAYERS * r.shape[1] * r.shape[2] for r in g)
    factor = jnp.minimum(1.0, 0.5 * lax.rsqrt(total[...] / count + 1e-30))[:1, :1]
    tenth = 0.1 * factor
    copies = []
    for k in range(3):
        rows = 16 * UPDATE_COLS // g[k].shape[2]
        steps = g[k].shape[1] // rows

        for layer in range(LAYERS):
            for half in range(UPDATE_PARTS):
                part = steps // UPDATE_PARTS

                @pl.loop(half * part, (half + 1) * part)
                def _(i):
                    at = (layer, pl.ds(pl.multiple_of(i * rows, rows), rows))
                    new_w[k][at], new_m[k][at], new_v[k][at] = adamw(w[k][at].astype(F32), m[k][at], v[k][at], g[k][at].astype(F32) * tenth)

                done = (layer, pl.ds(half * part * rows, part * rows))
                for new, out in ((new_m[k], out_m[k]), (new_v[k], out_v[k])):
                    copies.append(pltpu.make_async_copy(new.at[done], out.at[done], sem.at[len(copies)]))
                    copies[-1].start()
    for one in copies:
        one.wait()


def update(g, w, m, v, total):
    moments = [jax.ShapeDtypeStruct(one.shape, F32) for one in (*m, *v)]
    out = pl.pallas_call(
        update_kernel,
        out_shape=[pltpu.VMEM(one.shape, BF16) for one in w] + moments,
        in_specs=[pl.BlockSpec(memory_space=pltpu.VMEM)] * 13,
        out_specs=[pl.BlockSpec(memory_space=pltpu.VMEM)] * 3 + [pl.BlockSpec(memory_space=pltpu.HBM)] * 6,
        scratch_shapes=[pltpu.VMEM(one.shape, F32) for one in moments] + [pltpu.SemaphoreType.DMA((6 * LAYERS * UPDATE_PARTS,))],
        compiler_params=pltpu.CompilerParams(vmem_limit_bytes=14 * 2**20),
        name="update",
    )(*g, *w, *m, *v, total)
    return out[:3], out[3:6], out[6:]


def gather_kernel(*refs):
    w, refs = refs[:3], refs[3:]
    whole, (own_tx, own_rx, tx, rx, ftx, frx, last_tx, last_rx) = refs[:3], refs[3:]
    me = lax.axis_index("dp")
    bit, peer = place(me)
    heights = [r.shape[-2] // GATHER_CHUNKS for r in whole]

    def region(k, j, bits):
        h = heights[k]
        where = tuple(bits.get(a, slice(None)) for a in "xyz")
        return whole[k].at[(j // GATHER_CHUNKS, *where, bit["c"], pl.ds((j % GATHER_CHUNKS) * h, h))]

    def hop(k, stage, j):
        axes = ORDERS[k][: 3 - stage]
        part = region(k, j, {a: bit[a] for a in axes})
        if stage == 0:
            h = heights[k]
            source = w[k].at[j // GATHER_CHUNKS, pl.ds((j % GATHER_CHUNKS) * h, h)]
        else:
            source = part
        return send(source, part, (tx.at[stage, k, j], rx.at[stage, k, j]), peer[ORDERS[k][2 - stage]])

    def forward(k, stage, j):
        bits = {a: bit[a] for a in ORDERS[k][: 3 - stage]}
        axis = ORDERS[k][2 - stage]
        bits[axis] = 1 - bit[axis]
        part = region(k, j, bits)
        return send(part, part, (ftx.at[stage, k, j], frx.at[stage, k, j]), peer["c"])

    def last_hop(k, q, forward):
        axis = ORDERS[k][0]
        h = heights[k] // GATHER_TAIL if k == 2 else heights[k]
        w = whole[k].shape[-1] // (1 if k == 2 else GATHER_TAIL)
        row, col = (GATHER_CHUNKS - 1) * heights[k] + (q * h if k == 2 else 0), 0 if k == 2 else q * w
        where = tuple((1 - bit[axis] if forward else bit[axis]) if a == axis else slice(None) for a in "xyz")
        part = whole[k].at[(LAYERS - 1, *where, bit["c"], pl.ds(row, h), pl.ds(col, w))]
        way = int(forward)
        return send(part, part, (last_tx.at[way, k, q], last_rx.at[way, k, q]), peer["c" if forward else axis])

    def own_forward(k):
        part = whole[k].at[:, bit["x"], bit["y"], bit["z"], bit["c"]]
        return send(w[k], part, (own_tx.at[k], own_rx.at[k]), peer["c"])

    greet_near(peer)

    def first(j, _):
        for k in range(3):
            hop(k, 0, j).start()
        return 0

    lax.fori_loop(0, GATHER_JOBS, first, 0)
    for k in range(3):
        own_forward(k).start()
    for k in range(3):
        whole[k][:, bit["x"], bit["y"], bit["z"], bit["c"]] = w[k][...]

    def turn(s, _):
        for stage in range(3):
            end = GATHER_JOBS - 1 if stage == 2 else GATHER_JOBS

            @pl.when((s >= stage) & (s < end + stage))
            def _():
                j = s - stage
                for k in range(3):
                    hop(k, stage, j).wait_recv()
                    if stage == 0:
                        hop(k, 1, j).start()
                    if stage == 1:

                        @pl.when(j < GATHER_JOBS - 1)
                        def _():
                            hop(k, 2, j).start()

                        @pl.when(j == GATHER_JOBS - 1)
                        def _():
                            for q in range(GATHER_TAIL):
                                last_hop(k, q, False).start()

                    forward(k, stage, j).start()

        return 0

    lax.fori_loop(0, GATHER_JOBS + 1, turn, 0)
    for q in range(GATHER_TAIL):
        for k in range(3):
            last_hop(k, q, False).wait_recv()
            last_hop(k, q, True).start()

    def drain(j, _):
        for k in range(3):
            for stage in range(3):
                hop(k, stage, j).wait_send()
                forward(k, stage, j).wait()
        return 0

    lax.fori_loop(0, GATHER_JOBS - 1, drain, 0)
    for k in range(3):
        for stage in range(2):
            hop(k, stage, GATHER_JOBS - 1).wait_send()
            forward(k, stage, GATHER_JOBS - 1).wait()
        own_forward(k).wait()
        for q in range(GATHER_TAIL):
            last_hop(k, q, False).wait_send()
            last_hop(k, q, True).wait()


def land_kernel(*refs):
    held, out, sem = refs[:3], refs[3:6], refs[6]
    copies = [pltpu.make_async_copy(held[k].at[l, x], out[k].at[l, x], sem.at[k, l, x]) for k in range(3) for l in range(LAYERS) for x in range(2)]
    for one in copies:
        one.start()
    for one in copies:
        one.wait()


def gather(blocks):
    shapes = [b.shape[1:] for b in blocks]
    sem = pltpu.SemaphoreType.DMA
    whole = pl.pallas_call(
        gather_kernel,
        out_shape=[pltpu.VMEM((LAYERS, 2, 2, 2, 2, *s), BF16) for s in shapes],
        in_specs=[pl.BlockSpec(memory_space=pltpu.VMEM)] * 3,
        out_specs=[pl.BlockSpec(memory_space=pltpu.VMEM)] * 3,
        scratch_shapes=[sem((3,))] * 2 + [sem((3, 3, GATHER_JOBS))] * 4 + [sem((2, 3, GATHER_TAIL))] * 2,
        compiler_params=pltpu.CompilerParams(collective_id=1, has_side_effects=True, vmem_limit_bytes=2**20),
        name="gather",
    )(*blocks)
    landed = pl.pallas_call(
        land_kernel,
        out_shape=[jax.ShapeDtypeStruct(one.shape, BF16) for one in whole],
        in_specs=[pl.BlockSpec(memory_space=pltpu.VMEM)] * 3,
        out_specs=[pl.BlockSpec(memory_space=pltpu.HBM)] * 3,
        scratch_shapes=[sem((3, LAYERS, 2))],
        compiler_params=pltpu.CompilerParams(vmem_limit_bytes=LAND_VMEM),
        name="land",
    )(*whole)
    return [t.reshape(LAYERS, DEVICES * s[0], s[1]) for t, s in zip(landed, shapes, strict=True)]


def solution(mesh):
    def step(*arrays):
        terms, weights, m, v = (arrays[i : i + 3] for i in (0, 3, 6, 9))
        sums, total, own, m, v = scatter([t[0] for t in terms], weights, (*m, *v))
        new, m, v = update(sums, own, m, v, total)
        whole = gather(new)
        return (*whole, *m, *v)

    all_of, cut = P(None, None, None), P(None, "dp", None)
    return jax.shard_map(
        step,
        mesh=mesh,
        in_specs=(P(("rep", "dp"), None, None, None),) * 3 + (all_of,) * 3 + (cut,) * 6,
        out_specs=(P("rep", None, None),) * 3 + (P("rep", "dp", None),) * 6,
        check_vma=False,
    )
```

```python
import functools

import jax
import jax.numpy as jnp
from jax import lax
from jax.experimental import pallas as pl
from jax.experimental.pallas import tpu as pltpu
from jax.sharding import PartitionSpec as P

MESH = pl.DeviceIdType.MESH
BF16, F32 = jnp.bfloat16, jnp.float32
DEVICES = 16
LAYERS = 2
CHUNKS = 4
JOBS = LAYERS * CHUNKS
FINE = 4
ITEMS = JOBS - 1 + FINE
SLOTS, AHEAD = 5, 3
LAGS = (1, 3, 5)
GATHER_CHUNKS = 1
GATHER_TAIL = 8
GATHER_JOBS = LAYERS * GATHER_CHUNKS
SCATTER_VMEM, LAND_VMEM = 44_700_000, 4 * 2**20
UPDATE_COLS, UPDATE_PARTS = 4096, 2
ORDERS = ("xyz", "yzx", "zxy")
STEP = {"x": 8, "y": 4, "z": 2, "c": 1}


def adamw(w, m, v, h):
    m = 0.9 * m + h
    v = 0.95 * v + (5.0 * h) * h
    return (0.998 * w - (0.02 * m) * lax.rsqrt(v + 1e-8)).astype(jnp.bfloat16), m, v


def place(me):
    bit = {a: (me // s) % 2 for a, s in STEP.items()}
    peer = {a: me + s - 2 * s * bit[a] for a, s in STEP.items()}
    return bit, peer


def greet_near(peer, meanwhile=None):
    barrier = pltpu.get_barrier_semaphore()
    for one in peer.values():
        pl.semaphore_signal(barrier, inc=1, device_id={"dp": one}, device_id_type=MESH)
    if meanwhile:
        meanwhile()
    pl.semaphore_wait(barrier, len(peer))


def send(src, dst, sems, to):
    return pltpu.make_async_remote_copy(src, dst, sems[0], sems[1], device_id={"dp": to}, device_id_type=MESH)


def at_axis(ref, lead, axes, axis, bit):
    where = tuple(bit if a == axis else slice(None) for a in axes)
    return ref.at[(*lead, *where)]


def scatter_kernel(*refs):
    g, w, moments, refs = refs[:3], refs[3:6], refs[6:12], refs[12:]
    gb, total, own_w, held, refs = refs[:3], refs[3], refs[4:7], refs[7:13], refs[13:]
    own, s0, r1, r2, r3, acc = (refs[3 * i : 3 * i + 3] for i in range(6))
    mine, all_sq, own_sem, tx, rx, sq_tx, sq_rx, held_sem, free = refs[18:]
    me = lax.axis_index("dp")
    bit, peer = place(me)

    class Item:
        def __init__(self, i, fine):
            self.i, self.fine = i, fine
            self.j = 0 if fine else i - FINE + 1

        def part(self, k):
            h, w = r3[k].shape[-2:]
            if not self.fine:
                return pl.ds(0, h), pl.ds(0, w)
            if k == 2:
                return pl.ds(self.i * (h // FINE), h // FINE), pl.ds(0, w)
            return pl.ds(0, h), pl.ds(pl.multiple_of(self.i * (w // FINE), w // FINE), w // FINE)

        def piece(self, k):
            h = r3[k].shape[-2]
            rows, cols = self.part(k)
            return self.j // CHUNKS, pl.ds((self.j % CHUNKS) * h + rows.start, rows.size), cols

        def at(self, k, ref, lead, *where):
            return ref.at[(lead, *where, *self.part(k))]

        def own_copy(self, k):
            layer, rows, cols = self.piece(k)
            mine = self.at(k, own[k], self.i % 2, *[slice(None)] * 3)
            return pltpu.make_async_copy(g[k].at[layer, :, :, :, bit["c"], rows, cols], mine, own_sem.at[k, self.i])

        def hop(self, k, stage):
            sems = (tx.at[stage, k, self.i], rx.at[stage, k, self.i])
            a1, a2, a3 = ORDERS[k]
            every = slice(None)
            if stage == 0:
                layer, rows, cols = self.piece(k)
                theirs = self.at(k, s0[k], self.i % SLOTS, every, every, every)
                return send(g[k].at[layer, :, :, :, 1 - bit["c"], rows, cols], theirs, sems, peer["c"])
            if stage == 1:
                half = [1 - bit[a] if a == a1 else every for a in "xyz"]
                return send(self.at(k, s0[k], self.i % SLOTS, *half), self.at(k, r1[k], self.j, every, every), sems, peer[a1])
            if stage == 2:
                half = [1 - bit[a] if a == a2 else every for a in "xyz" if a != a1]
                return send(self.at(k, r1[k], self.j, *half), self.at(k, r2[k], self.j, every), sems, peer[a2])
            return send(self.at(k, r2[k], self.j, 1 - bit[a3]), self.at(k, r3[k], self.j), sems, peer[a3])

        def fetch(self):
            for k in range(3):
                self.own_copy(k).start()

        def cross(self):
            for k in range(3):
                self.hop(k, 0).start()

        def add_core(self):
            for k in range(3):
                self.own_copy(k).wait()
                self.hop(k, 0).wait_recv()

                @pl.loop(0, 2 if self.fine else 8)
                def _(b):
                    at = (b, slice(None), slice(None)) if self.fine else (b // 4, (b // 2) % 2, b % 2)
                    at = (*at, *self.part(k))
                    slot = (self.i % SLOTS, *at)
                    s0[k][slot] = plus(own[k][(self.i % 2, *at)], s0[k][slot])

                self.hop(k, 1).start()

        def add_first(self):
            for k in range(3):
                a1 = ORDERS[k][0]
                self.hop(k, 1).wait_recv()

                @pl.loop(0, 2 if self.fine else 4)
                def _(b):
                    at = [b, slice(None)] if self.fine else [b // 2, b % 2]
                    full = list(at)
                    full.insert("xyz".index(a1), bit[a1])
                    to = (self.j, *at, *self.part(k))
                    r1[k][to] = plus(s0[k][(self.i % SLOTS, *full, *self.part(k))], r1[k][to])

                self.hop(k, 2).start()
            for k in range(3):
                self.hop(k, 1).wait_send()

        def add_second(self):
            for k in range(3):
                a1, a2, _a3 = ORDERS[k]
                rest = [a for a in "xyz" if a != a1]
                self.hop(k, 2).wait_recv()

                @pl.loop(0, 2)
                def _(b):
                    full = [b]
                    full.insert(rest.index(a2), bit[a2])
                    to = (self.j, b, *self.part(k))
                    r2[k][to] = plus(r1[k][(self.j, *full, *self.part(k))], r2[k][to])

                self.hop(k, 3).start()

        def add_third(self):
            for k in range(3):
                self.hop(k, 3).wait_recv()
                done = plus(r2[k][(self.j, bit[ORDERS[k][2]], *self.part(k))], r3[k][(self.j, *self.part(k))])
                gb[k][self.piece(k)] = done
                wide = done.astype(F32)
                squares = wide * wide
                low = sum(squares[8 * i : 8 * i + 8] for i in range(done.shape[0] // 8))
                acc[k][...] += sum(low[:, 128 * i : 128 * i + 128] for i in range(low.shape[1] // 128))

        def drain(self):
            for k in range(3):
                for stage in (0, 2, 3):
                    self.hop(k, stage).wait_send()

    def plus(a, b):
        return (a.astype(F32) + b.astype(F32)).astype(BF16)

    def do(i, what):
        @pl.when((i >= 0) & (i < FINE))
        def _():
            getattr(Item(i, True), what)()

        @pl.when((i >= FINE) & (i < ITEMS))
        def _():
            getattr(Item(i, False), what)()

    staged = [pltpu.make_async_copy(w[k].at[:, bit["x"], bit["y"], bit["z"], bit["c"]], own_w[k], held_sem.at[k]) for k in range(3)]
    staged += [pltpu.make_async_copy(moments[i], held[i], held_sem.at[3 + i]) for i in range(6)]

    greet_near(peer, Item(0, True).fetch)
    for i in range(AHEAD):
        Item(i, True).cross()
    for k in range(3):
        acc[k][...] = jnp.zeros_like(acc[k])

    def turn(s, _):
        @pl.when((s >= SLOTS - AHEAD) & (s < ITEMS - AHEAD))
        def _():
            pl.semaphore_wait(free, 1)

        do(s + AHEAD, "cross")
        do(s + 1, "fetch")

        @pl.when(s == FINE)
        def _():
            for one in staged:
                one.start()

        do(s, "add_core")
        do(s - LAGS[0], "add_first")

        @pl.when((s >= LAGS[0]) & (s < LAGS[0] + ITEMS - SLOTS))
        def _():
            pl.semaphore_signal(free, inc=1, device_id={"dp": peer["c"]}, device_id_type=MESH)

        do(s - LAGS[1], "add_second")
        do(s - LAGS[2], "add_third")
        return 0

    lax.fori_loop(0, ITEMS + LAGS[2], turn, 0)

    part = jnp.zeros((8, 128), F32)
    for k in range(3):
        part += acc[k][...]
    part = jnp.sum(part, axis=0, keepdims=True)
    mine[...] = part
    all_sq[me] = part
    sends = [send(mine, all_sq.at[me], (sq_tx.at[i], sq_rx.at[i]), (me + i) % DEVICES) for i in range(1, DEVICES)]
    for one in sends:
        one.start()

    def drain(i, _):
        do(i, "drain")
        return 0

    lax.fori_loop(0, ITEMS, drain, 0)
    for one in staged:
        one.wait()
    for one in sends:
        one.wait()
    total[...] = jnp.full((8, 128), jnp.sum(sum(all_sq[i] for i in range(DEVICES))), F32)


def scatter(terms, weights, moments):
    blocks = [(t.shape[1] // DEVICES, t.shape[2]) for t in terms]
    split = [t.reshape(LAYERS, 2, 2, 2, 2, *b) for t, b in zip((*terms, *weights), (*blocks, *blocks), strict=True)]
    pieces = [(r // CHUNKS, c) for r, c in blocks]
    sem = pltpu.SemaphoreType.DMA
    leads = ((2, 2, 2, 2), (SLOTS, 2, 2, 2), (JOBS, 2, 2), (JOBS, 2), (JOBS,))
    scratch = [pltpu.VMEM((*lead, *p), BF16) for lead in leads for p in pieces]
    scratch += [pltpu.VMEM((8, 128), F32)] * 3
    scratch += [pltpu.VMEM((1, 128), F32), pltpu.VMEM((DEVICES, 1, 128), F32)]
    scratch += [sem((3, ITEMS)), sem((4, 3, ITEMS)), sem((4, 3, ITEMS)), sem((DEVICES,)), sem((DEVICES,)), sem((9,)), pltpu.SemaphoreType.REGULAR]
    sums_0, sums_1, sums_2, total, *held = pl.pallas_call(
        scatter_kernel,
        out_shape=[pltpu.VMEM((LAYERS, *b), BF16) for b in blocks] + [pltpu.VMEM((8, 128), F32)] + [pltpu.VMEM((LAYERS, *b), BF16) for b in blocks] + [pltpu.VMEM(m.shape, F32) for m in moments],
        in_specs=[pl.BlockSpec(memory_space=pltpu.HBM)] * 12,
        out_specs=[pl.BlockSpec(memory_space=pltpu.VMEM)] * 13,
        scratch_shapes=scratch,
        compiler_params=pltpu.CompilerParams(collective_id=0, has_side_effects=True, vmem_limit_bytes=SCATTER_VMEM),
        name="scatter",
    )(*split, *moments)
    return (sums_0, sums_1, sums_2), total, held[:3], held[3:6], held[6:]


def update_kernel(*refs):
    g, w, m, v, total = refs[:3], refs[3:6], refs[6:9], refs[9:12], refs[12]
    new_w, out_m, out_v, refs = refs[13:16], refs[16:19], refs[19:22], refs[22:]
    new_m, new_v, sem = refs[:3], refs[3:6], refs[6]
    count = DEVICES * sum(LAYERS * r.shape[1] * r.shape[2] for r in g)
    factor = jnp.minimum(1.0, 0.5 * lax.rsqrt(total[...] / count + 1e-30))[:1, :1]
    tenth = 0.1 * factor
    copies = []
    for k in range(3):
        rows = 16 * UPDATE_COLS // g[k].shape[2]
        steps = g[k].shape[1] // rows

        for layer in range(LAYERS):
            for half in range(UPDATE_PARTS):
                part = steps // UPDATE_PARTS

                @pl.loop(half * part, (half + 1) * part)
                def _(i):
                    at = (layer, pl.ds(pl.multiple_of(i * rows, rows), rows))
                    new_w[k][at], new_m[k][at], new_v[k][at] = adamw(w[k][at].astype(F32), m[k][at], v[k][at], g[k][at].astype(F32) * tenth)

                done = (layer, pl.ds(half * part * rows, part * rows))
                for new, out in ((new_m[k], out_m[k]), (new_v[k], out_v[k])):
                    copies.append(pltpu.make_async_copy(new.at[done], out.at[done], sem.at[len(copies)]))
                    copies[-1].start()
    for one in copies:
        one.wait()


def update(g, w, m, v, total):
    moments = [jax.ShapeDtypeStruct(one.shape, F32) for one in (*m, *v)]
    out = pl.pallas_call(
        update_kernel,
        out_shape=[pltpu.VMEM(one.shape, BF16) for one in w] + moments,
        in_specs=[pl.BlockSpec(memory_space=pltpu.VMEM)] * 13,
        out_specs=[pl.BlockSpec(memory_space=pltpu.VMEM)] * 3 + [pl.BlockSpec(memory_space=pltpu.HBM)] * 6,
        scratch_shapes=[pltpu.VMEM(one.shape, F32) for one in moments] + [pltpu.SemaphoreType.DMA((6 * LAYERS * UPDATE_PARTS,))],
        compiler_params=pltpu.CompilerParams(vmem_limit_bytes=14 * 2**20),
        name="update",
    )(*g, *w, *m, *v, total)
    return out[:3], out[3:6], out[6:]


def gather_kernel(*refs):
    w, refs = refs[:3], refs[3:]
    whole, (own_tx, own_rx, tx, rx, ftx, frx, last_tx, last_rx) = refs[:3], refs[3:]
    me = lax.axis_index("dp")
    bit, peer = place(me)
    heights = [r.shape[-2] // GATHER_CHUNKS for r in whole]

    def region(k, j, bits):
        h = heights[k]
        where = tuple(bits.get(a, slice(None)) for a in "xyz")
        return whole[k].at[(j // GATHER_CHUNKS, *where, bit["c"], pl.ds((j % GATHER_CHUNKS) * h, h))]

    def hop(k, stage, j):
        axes = ORDERS[k][: 3 - stage]
        part = region(k, j, {a: bit[a] for a in axes})
        if stage == 0:
            h = heights[k]
            source = w[k].at[j // GATHER_CHUNKS, pl.ds((j % GATHER_CHUNKS) * h, h)]
        else:
            source = part
        return send(source, part, (tx.at[stage, k, j], rx.at[stage, k, j]), peer[ORDERS[k][2 - stage]])

    def forward(k, stage, j):
        bits = {a: bit[a] for a in ORDERS[k][: 3 - stage]}
        axis = ORDERS[k][2 - stage]
        bits[axis] = 1 - bit[axis]
        part = region(k, j, bits)
        return send(part, part, (ftx.at[stage, k, j], frx.at[stage, k, j]), peer["c"])

    def last_hop(k, q, forward):
        axis = ORDERS[k][0]
        h = heights[k] // GATHER_TAIL if k == 2 else heights[k]
        w = whole[k].shape[-1] // (1 if k == 2 else GATHER_TAIL)
        row, col = (GATHER_CHUNKS - 1) * heights[k] + (q * h if k == 2 else 0), 0 if k == 2 else q * w
        where = tuple((1 - bit[axis] if forward else bit[axis]) if a == axis else slice(None) for a in "xyz")
        part = whole[k].at[(LAYERS - 1, *where, bit["c"], pl.ds(row, h), pl.ds(col, w))]
        way = int(forward)
        return send(part, part, (last_tx.at[way, k, q], last_rx.at[way, k, q]), peer["c" if forward else axis])

    def own_forward(k):
        part = whole[k].at[:, bit["x"], bit["y"], bit["z"], bit["c"]]
        return send(w[k], part, (own_tx.at[k], own_rx.at[k]), peer["c"])

    greet_near(peer)

    def first(j, _):
        for k in range(3):
            hop(k, 0, j).start()
        return 0

    lax.fori_loop(0, GATHER_JOBS, first, 0)
    for k in range(3):
        own_forward(k).start()
    for k in range(3):
        whole[k][:, bit["x"], bit["y"], bit["z"], bit["c"]] = w[k][...]

    def turn(s, _):
        for stage in range(3):
            end = GATHER_JOBS - 1 if stage == 2 else GATHER_JOBS

            @pl.when((s >= stage) & (s < end + stage))
            def _():
                j = s - stage
                for k in range(3):
                    hop(k, stage, j).wait_recv()
                    if stage == 0:
                        hop(k, 1, j).start()
                    if stage == 1:

                        @pl.when(j < GATHER_JOBS - 1)
                        def _():
                            hop(k, 2, j).start()

                        @pl.when(j == GATHER_JOBS - 1)
                        def _():
                            for q in range(GATHER_TAIL):
                                last_hop(k, q, False).start()

                    forward(k, stage, j).start()

        return 0

    lax.fori_loop(0, GATHER_JOBS + 1, turn, 0)
    for q in range(GATHER_TAIL):
        for k in range(3):
            last_hop(k, q, False).wait_recv()
            last_hop(k, q, True).start()

    def drain(j, _):
        for k in range(3):
            for stage in range(3):
                hop(k, stage, j).wait_send()
                forward(k, stage, j).wait()
        return 0

    lax.fori_loop(0, GATHER_JOBS - 1, drain, 0)
    for k in range(3):
        for stage in range(2):
            hop(k, stage, GATHER_JOBS - 1).wait_send()
            forward(k, stage, GATHER_JOBS - 1).wait()
        own_forward(k).wait()
        for q in range(GATHER_TAIL):
            last_hop(k, q, False).wait_send()
            last_hop(k, q, True).wait()


def land_kernel(*refs):
    held, out, sem = refs[:3], refs[3:6], refs[6]
    copies = [pltpu.make_async_copy(held[k].at[l, x], out[k].at[l, x], sem.at[k, l, x]) for k in range(3) for l in range(LAYERS) for x in range(2)]
    for one in copies:
        one.start()
    for one in copies:
        one.wait()


def gather(blocks):
    shapes = [b.shape[1:] for b in blocks]
    sem = pltpu.SemaphoreType.DMA
    whole = pl.pallas_call(
        gather_kernel,
        out_shape=[pltpu.VMEM((LAYERS, 2, 2, 2, 2, *s), BF16) for s in shapes],
        in_specs=[pl.BlockSpec(memory_space=pltpu.VMEM)] * 3,
        out_specs=[pl.BlockSpec(memory_space=pltpu.VMEM)] * 3,
        scratch_shapes=[sem((3,))] * 2 + [sem((3, 3, GATHER_JOBS))] * 4 + [sem((2, 3, GATHER_TAIL))] * 2,
        compiler_params=pltpu.CompilerParams(collective_id=1, has_side_effects=True, vmem_limit_bytes=2**20),
        name="gather",
    )(*blocks)
    landed = pl.pallas_call(
        land_kernel,
        out_shape=[jax.ShapeDtypeStruct(one.shape, BF16) for one in whole],
        in_specs=[pl.BlockSpec(memory_space=pltpu.VMEM)] * 3,
        out_specs=[pl.BlockSpec(memory_space=pltpu.HBM)] * 3,
        scratch_shapes=[sem((3, LAYERS, 2))],
        compiler_params=pltpu.CompilerParams(vmem_limit_bytes=LAND_VMEM),
        name="land",
    )(*whole)
    return [t.reshape(LAYERS, DEVICES * s[0], s[1]) for t, s in zip(landed, shapes, strict=True)]


def solution(mesh):
    def step(*arrays):
        terms, weights, m, v = (arrays[i : i + 3] for i in (0, 3, 6, 9))
        sums, total, own, m, v = scatter([t[0] for t in terms], weights, (*m, *v))
        new, m, v = update(sums, own, m, v, total)
        whole = gather(new)
        return (*whole, *m, *v)

    all_of, cut = P(None, None, None), P(None, "dp", None)
    return jax.shard_map(
        step,
        mesh=mesh,
        in_specs=(P(("rep", "dp"), None, None, None),) * 3 + (all_of,) * 3 + (cut,) * 6,
        out_specs=(P("rep", None, None),) * 3 + (P("rep", "dp", None),) * 6,
        check_vma=False,
    )
```
